32 devices in a mesh: cp: 8 (over z, x), tp: 4 (over y, core).
Axes of the slice: x: 2, y: 2, z: 4, core: 2. Of those that a mesh axis runs over, the one named last changes fastest.
Arguments:
- queries: bfloat16 [1024, 8192], P('cp', 'tp'), may hold values from -6 to 6
- keys: bfloat16 [1024, 1024], P('cp', 'tp'), may hold values from -6 to 6
- values: bfloat16 [1024, 1024], P('cp', 'tp'), may hold values from -6 to 6
- doc_blocks: int32 [4], replicated, may hold values from 1 to 4, 8 in all
- block_order: int32 [8], replicated, may hold values from 0 to 7, each once
- out_weight: bfloat16 [8192, 4096], P('tp'), may hold values from -0.5 to 0.5
Outputs:
- layer_out: bfloat16 [1024, 4096], P(('cp', 'tp'))
The draws below stay inside these ranges and needn't reach their ends.
Inputs may be any that keep to these rules, and one draw needn't show every extreme that they name: Array block i (rows i * 128 to i * 128 + 127) holds sequence block block_order[i]; every block number appears once. `doc_blocks`: they sum to 8; the longest document has exactly 4 blocks.
All inputs are finite; a program needn't handle non-finite values.
Results may differ from the reference program's by a relative error of at most 0.013.
Values may be sent and summed in bfloat16 or wider, within the bound.
No kernel may reach another device: no remote copies, remote signals or barrier semaphores. Data moves between devices by JAX's collectives and lax.ppermute only.
A program may use at most 128 MiB of HBM per device.

```python
import math
import jax
import jax.numpy as jnp
import numpy as np
from jax import lax

QUERY_HEADS = 64
KEY_VALUE_HEADS = 8
HEAD_SIZE = 128
WIN = 4096
BLOCK_TOKENS = 128
NDOC = 4
GROUP_HEADS = 8
PACK_TOKENS = 1024
NBLK = 8
MOSTB = 4


def draw_keys(key, part):
    picked_rows = jax.random.truncated_normal(jax.random.fold_in(key, 13), -4.0, 4.0, (PACK_TOKENS, KEY_VALUE_HEADS * HEAD_SIZE), jnp.float32)
    return picked_rows.astype(jnp.bfloat16)


def draw_queries(key, part):
    picked_rows = jax.random.truncated_normal(jax.random.fold_in(key, 14), -4.0, 4.0, (PACK_TOKENS, QUERY_HEADS * HEAD_SIZE), jnp.float32)
    return picked_rows.astype(jnp.bfloat16)


def level_of(own_key, dims, pieces, smallest, top_value):
    factor_of, own = 1.0, jax.random.fold_in(own_key, 6)
    for dim, blocks in pieces:
        heights = jnp.exp(jax.random.uniform(jax.random.fold_in(own, dim), (blocks,), jnp.float32, smallest / len(pieces), top_value / len(pieces)))
        factor_of = factor_of * jnp.repeat(heights, dims[dim] // blocks).reshape([-1 if axis == dim else 1 for axis in range(len(dims))])
    return factor_of


def split_up(count, total, most, slope):
    weights = [(1 << 20) // math.isqrt(standing ** slope) + 1 for standing in range(2, count + 1)]
    surplus, counts = total - most - (count - 1), [1] * (count - 1)
    while surplus > 0:
        movable = [i for i in range(count - 1) if counts[i] < most]
        mass, remaining = sum([weights[i] for i in movable]), surplus
        for i in movable:
            extra = min(most - counts[i], max(1, remaining * weights[i] // mass), surplus)
            counts[i] = counts[i] + extra
            surplus = surplus - extra
    return np.array([most] + counts)


def uneven_parts(stream_key, amount, total, reach, lean):
    if amount == 2:
        one = jax.random.randint(stream_key, (), max(1, total - reach), min(reach, total - 1) + 1)
        return jnp.stack([one, total - one])
    tallies = jnp.asarray(split_up(amount, total, reach, lean), jnp.int32)
    pairs = (amount - 1) // 2
    giver, sink = tallies[1:1 + 2 * pairs:2], tallies[2:2 + 2 * pairs:2]
    margin = jnp.minimum(giver - 1, reach - sink)
    passed = jax.random.randint(jax.random.fold_in(stream_key, 1), (pairs,), 0, 1 << 20) % (margin + 1)
    tallies = tallies.at[1:1 + 2 * pairs:2].set(giver - passed).at[2:2 + 2 * pairs:2].set(sink + passed)
    return tallies[jax.random.permutation(jax.random.fold_in(stream_key, 2), amount)]


def scatter_about(rng, shape, scale, bound, shards=(), kind=jnp.bfloat16):
    level = level_of(rng, shape, shards, -0.22, 0.18) if shards else 1.0
    values = jax.random.normal(rng, shape, jnp.float32) * scale * level
    return jnp.minimum(jnp.maximum(values, -bound), bound).astype(kind)


def setup_inputs(seed: int = 0) -> dict:
    arg_keys = jax.random.split(jax.random.key(seed), 7)
    queries = draw_queries(jax.random.fold_in(arg_keys[6], 71), 0)
    keys = draw_keys(jax.random.fold_in(arg_keys[6], 71), 0)
    values = scatter_about(arg_keys[2], (PACK_TOKENS, KEY_VALUE_HEADS * HEAD_SIZE), 1.0, 6.0, ((0, 8), (1, 4)))
    doc_blocks = uneven_parts(arg_keys[3], NDOC, NBLK, MOSTB, 2).astype(jnp.int32)
    block_order = jax.random.permutation(arg_keys[4], NBLK).astype(jnp.int32)
    out_weight = scatter_about(arg_keys[5], (QUERY_HEADS * HEAD_SIZE, WIN), HEAD_SIZE ** -0.5, 0.5, ((0, 4),))
    return dict(queries=queries, keys=keys, values=values, doc_blocks=doc_blocks, block_order=block_order, out_weight=out_weight)


document_masked_score = -1.0e30


def reference(queries, keys, values, doc_blocks, block_order, out_weight):
    token_blocks = PACK_TOKENS // BLOCK_TOKENS
    block_ids = jnp.arange(token_blocks, dtype=jnp.int32)
    inverse_order = jnp.zeros((token_blocks,), jnp.int32).at[block_order].set(block_ids)
    sequence_queries = queries.reshape(token_blocks, BLOCK_TOKENS, KEY_VALUE_HEADS, GROUP_HEADS, HEAD_SIZE)[inverse_order]
    sequence_keys = keys.reshape(token_blocks, BLOCK_TOKENS, KEY_VALUE_HEADS, HEAD_SIZE)[inverse_order]
    sequence_values = values.reshape(token_blocks, BLOCK_TOKENS, KEY_VALUE_HEADS, HEAD_SIZE)[inverse_order]
    doc_ends = jnp.cumsum(doc_blocks).astype(jnp.int32)
    doc_of = jnp.sum((block_ids[:, None] >= doc_ends[None, :]).astype(jnp.int32), axis=1)
    doc_first = (doc_ends - doc_blocks).astype(jnp.int32)[doc_of]
    inner = jnp.arange(BLOCK_TOKENS, dtype=jnp.int32)

    def one_block(seq_block):
        query_rows = sequence_queries[seq_block].astype(jnp.float32)

        def add_tile(key_block, online):
            running_max, weight_sum, weighted = online
            key_rows = sequence_keys[key_block].astype(jnp.float32)
            value_rows = sequence_values[key_block].astype(jnp.float32)
            scores = jnp.einsum('qhgd,khd->hgqk', query_rows, key_rows) * (HEAD_SIZE ** -0.5)
            allowed = (key_block * BLOCK_TOKENS + inner[None, :]) <= (seq_block * BLOCK_TOKENS + inner[:, None])
            scores = jnp.where(allowed, scores, document_masked_score)
            new_max = jnp.maximum(running_max, jnp.max(scores, axis=-1))
            weights = jnp.where(allowed, jnp.exp(scores - new_max[..., None]), 0.0)
            factor = jnp.exp(running_max - new_max)
            weight_sum = weight_sum * factor + jnp.sum(weights, axis=-1)
            rounded = lax.optimization_barrier(weights.astype(jnp.bfloat16)).astype(jnp.float32)
            weighted = weighted * factor[..., None] + jnp.einsum('hgqk,khd->hgqd', rounded, value_rows)
            return new_max, weight_sum, weighted

        starting_state = (jnp.full((KEY_VALUE_HEADS, GROUP_HEADS, BLOCK_TOKENS), document_masked_score, jnp.float32),
                   jnp.zeros((KEY_VALUE_HEADS, GROUP_HEADS, BLOCK_TOKENS), jnp.float32),
                   jnp.zeros((KEY_VALUE_HEADS, GROUP_HEADS, BLOCK_TOKENS, HEAD_SIZE), jnp.float32))
        running_max, weight_sum, weighted = lax.fori_loop(doc_first[seq_block], seq_block + 1, add_tile, starting_state)
        result = weighted / weight_sum[..., None]
        return jnp.transpose(result, (2, 0, 1, 3)).reshape(BLOCK_TOKENS, QUERY_HEADS * HEAD_SIZE).astype(jnp.bfloat16)

    attended_seq = lax.map(one_block, block_ids)
    attended = attended_seq[block_order].reshape(PACK_TOKENS, QUERY_HEADS * HEAD_SIZE)
    return jnp.dot(attended, out_weight, preferred_element_type=jnp.float32).astype(jnp.bfloat16)
```

```python
import functools

import jax
import jax.numpy as jnp
from jax import lax
from jax.experimental import pallas as pl
from jax.experimental.pallas import tpu as pltpu
from jax.sharding import PartitionSpec as P

HEAD_SIZE = 128
BLOCK_TOKENS = 128
MASKED = -1e30


def lookup(entries, indices):
    matches = indices[:, None] == jnp.arange(entries.shape[0], dtype=jnp.int32)[None, :]
    return jnp.sum(jnp.where(matches, entries[None, :], 0), axis=1)


def locate(row_ids, block_order, doc_ends):
    seq_block = lookup(block_order, row_ids // BLOCK_TOKENS)
    position = seq_block * BLOCK_TOKENS + row_ids % BLOCK_TOKENS
    doc_ids = jnp.sum((seq_block[:, None] >= doc_ends[None, :]).astype(jnp.int32), axis=1)
    return (position, doc_ids)


def attend(online, key_rows, value_rows, key_pos, key_doc, query_rows, query_pos, query_doc):
    allowed = (query_doc[:, None] == key_doc[None, :]) & (key_pos[None, :] <= query_pos[:, None])
    running_max, weight_sum, weighted = online
    scores = jnp.einsum(
        "qhgd,khd->hgqk", query_rows, key_rows, preferred_element_type=jnp.float32
    ) * HEAD_SIZE ** (-0.5)
    scores = jnp.where(allowed, scores, MASKED)
    new_max = jnp.maximum(running_max, jnp.max(scores, axis=-1))
    weights = jnp.where(allowed, jnp.exp(scores - new_max[..., None]), 0.0)
    factor = jnp.exp(running_max - new_max)
    weight_sum = weight_sum * factor + jnp.sum(weights, axis=-1)
    weighted = weighted * factor[..., None] + jnp.einsum(
        "hgqk,khd->hgqd",
        weights.astype(jnp.bfloat16),
        value_rows,
        preferred_element_type=jnp.float32,
    )
    return (new_max, weight_sum, weighted)


def sweep_keys(
    online, key_part, value_part, block_order, doc_ends, query_rows, query_pos, query_doc
):
    length = key_part.shape[0]
    heads_kv = key_part.shape[1] // HEAD_SIZE
    block_rows = 4 * BLOCK_TOKENS
    token_blocks = length // block_rows
    key_pos, key_doc = locate(jnp.arange(length, dtype=jnp.int32), block_order, doc_ends)

    def scan_step(status, pieces_now):
        return attend(status, *pieces_now, query_rows, query_pos, query_doc), None

    online, unused = lax.scan(
        scan_step,
        online,
        (
            key_part.reshape(token_blocks, block_rows, heads_kv, HEAD_SIZE),
            value_part.reshape(token_blocks, block_rows, heads_kv, HEAD_SIZE),
            key_pos.reshape(token_blocks, block_rows),
            key_doc.reshape(token_blocks, block_rows),
        ),
    )
    return online


def general(queries, keys, values, doc_blocks, block_order, out_weight):
    rows_dev = queries.shape[0]
    heads_kv = keys.shape[1] // HEAD_SIZE
    group_size = queries.shape[1] // keys.shape[1]
    doc_ends = jnp.cumsum(doc_blocks)
    first_row = lax.axis_index("cp") * rows_dev
    query_pos, query_doc = locate(
        first_row + jnp.arange(rows_dev, dtype=jnp.int32), block_order, doc_ends
    )
    query_rows = queries.reshape(rows_dev, heads_kv, group_size, HEAD_SIZE)
    starting_state = (
        jnp.full((heads_kv, group_size, rows_dev), MASKED, jnp.float32),
        jnp.zeros((heads_kv, group_size, rows_dev), jnp.float32),
        jnp.zeros((heads_kv, group_size, rows_dev, HEAD_SIZE), jnp.float32),
    )
    whole_keys = lax.all_gather(keys, "cp", axis=0, tiled=True)
    whole_values = lax.all_gather(values, "cp", axis=0, tiled=True)
    running_max, weight_sum, weighted = sweep_keys(
        starting_state, whole_keys, whole_values, block_order, doc_ends,
        query_rows, query_pos, query_doc,
    )
    attended = (
        jnp.transpose(weighted / weight_sum[..., None], (2, 0, 1, 3))
        .reshape(rows_dev, -1)
        .astype(jnp.bfloat16)
    )
    return lax.psum_scatter(
        jnp.dot(attended, out_weight, preferred_element_type=jnp.float32).astype(jnp.bfloat16),
        "tp",
        scatter_dimension=0,
        tiled=True,
    )


def attend_project(n_blocks, n_tp, order_ref, docs_ref, q_ref, *refs):
    kv_refs, (w_hbm, give_ref, keep_ref, w_ref, kv_ref, att_ref, bias_ref, seq_ref, sems) = (
        refs[:n_blocks], refs[n_blocks:])
    n_docs = docs_ref.shape[0]
    n_slots = kv_ref.shape[0]
    n_chunks, _, chunk = w_ref.shape
    rows, width = q_ref.shape
    part = rows // n_tp
    heads_kv = kv_refs[0].shape[1] // HEAD_SIZE
    group = width // HEAD_SIZE // heads_kv
    me, core = lax.axis_index("cp"), lax.axis_index("tp")

    loads = [
        pltpu.make_async_copy(w_hbm.at[:, pl.ds(j * chunk, chunk)], w_ref.at[j], sems.at[j])
        for j in range(n_chunks)
    ]
    for load in loads:
        load.start()

    ends = []
    for d in range(n_docs):
        ends.append(docs_ref[d] + (ends[-1] if ends else 0))

    def document(seq):
        return sum((seq >= end).astype(jnp.int32) for end in ends)

    own_seq = order_ref[me]
    own_doc = document(own_seq)
    for slot in range(n_slots):
        kv_ref[slot] = kv_refs[0][...]
        seq_ref[slot] = own_seq if slot == 0 else own_seq + 1
    used = jnp.int32(1)
    for s in range(1, n_blocks):
        seq = order_ref[me ^ s]
        wanted = (document(seq) == own_doc) & (seq < own_seq)

        @pl.when(wanted)
        def _(s=s, seq=seq, used=used):
            kv_ref[used] = kv_refs[s][...]
            seq_ref[used] = seq

        used = used + wanted.astype(jnp.int32)

    targets = [core ^ f for f in (3, 1, 2, 0)]
    key_at = lax.broadcasted_iota(jnp.int32, (part, BLOCK_TOKENS), 1)
    row_at = lax.broadcasted_iota(jnp.int32, (part, BLOCK_TOKENS), 0)
    for slot in range(n_slots):
        ahead = (own_seq - seq_ref[slot]) * BLOCK_TOKENS
        for p, target in enumerate(targets):
            bias_ref[p * part : (p + 1) * part, slot * BLOCK_TOKENS : (slot + 1) * BLOCK_TOKENS] = (
                jnp.where(key_at <= row_at + (target * part + ahead), 0.0, MASKED)
            )

    def query(h):
        return [
            q_ref[pl.ds(pl.multiple_of(t * part, part), part), h * HEAD_SIZE : (h + 1) * HEAD_SIZE]
            for t in targets
        ]

    scale = HEAD_SIZE**-0.5 * 1.4426950408889634
    ones = jnp.ones((n_slots * BLOCK_TOKENS, HEAD_SIZE), jnp.bfloat16)
    for g in range(heads_kv):
        cols = slice(g * HEAD_SIZE, (g + 1) * HEAD_SIZE)
        key_rows = jnp.concatenate([kv_ref[j, :BLOCK_TOKENS, cols] for j in range(n_slots)], 0)
        value_rows = jnp.concatenate([kv_ref[j, BLOCK_TOKENS:, cols] for j in range(n_slots)], 0)
        value_rows = jnp.concatenate([value_rows, ones], 1)
        for h in range(g * group, (g + 1) * group):
            scores = lax.dot_general(
                jnp.concatenate(query(h), 0), key_rows, (((1,), (1,)), ((), ())),
                preferred_element_type=jnp.float32,
            ) + bias_ref[...]
            top = jnp.max(scores, axis=1, keepdims=True)
            weights = jnp.exp2((scores - top) * scale).astype(jnp.bfloat16)
            sums = jnp.dot(weights, value_rows, preferred_element_type=jnp.float32)
            att_ref[:, h * HEAD_SIZE : (h + 1) * HEAD_SIZE] = (
                sums[:, :HEAD_SIZE] / sums[:, HEAD_SIZE:]
            ).astype(jnp.bfloat16)

    half = rows // 2
    for j, load in enumerate(loads):
        load.wait()
        product = jnp.dot(att_ref[...], w_ref[j], preferred_element_type=jnp.float32)
        give_ref[:, j * chunk : (j + 1) * chunk] = product[:half].astype(jnp.bfloat16)
        keep_ref[:, j * chunk : (j + 1) * chunk] = product[half:]


def exchange(kv, n):
    def swap(block, s):
        return lax.ppermute(block, "cp", [(i, i ^ s) for i in range(n)])

    got = {0: kv}
    for s in range(2, n, 2):
        got[s] = swap(kv, s)
    for s in range(0, n, 2):
        got[s + 1] = swap(got[s], 1)
    return [got[s] for s in range(n)]


def blockwise(n, n_tp, queries, keys, values, doc_blocks, block_order, out_weight):
    rows, width = queries.shape
    out_width = out_weight.shape[1]
    blocks = exchange(jnp.concatenate([keys, values], 0), n)
    n_slots = n // 2
    chunk = out_width // 8
    smem = pl.BlockSpec(memory_space=pltpu.SMEM)
    vmem = pl.BlockSpec(memory_space=pltpu.VMEM)
    give, keep = pl.pallas_call(
        functools.partial(attend_project, n, n_tp),
        out_shape=(
            jax.ShapeDtypeStruct((rows // 2, out_width), jnp.bfloat16),
            jax.ShapeDtypeStruct((rows // 2, out_width), jnp.float32),
        ),
        in_specs=[smem, smem] + [vmem] * (n + 1) + [pl.BlockSpec(memory_space=pltpu.HBM)],
        out_specs=(vmem, vmem),
        scratch_shapes=[
            pltpu.VMEM((8, width, chunk), jnp.bfloat16),
            pltpu.VMEM((n_slots,) + blocks[0].shape, jnp.bfloat16),
            pltpu.VMEM((rows, width), jnp.bfloat16),
            pltpu.VMEM((rows, n_slots * BLOCK_TOKENS), jnp.float32),
            pltpu.SMEM((n_slots,), jnp.int32),
            pltpu.SemaphoreType.DMA((8,)),
        ],
        compiler_params=pltpu.CompilerParams(vmem_limit_bytes=40 * 1024 * 1024),
        cost_estimate=pl.CostEstimate(
            flops=2 * rows * width * out_width, bytes_accessed=2 * width * out_width,
            transcendentals=0),
        name="attend_project",
    )(block_order, doc_blocks, queries, *blocks, out_weight)
    part = rows // n_tp
    got = lax.ppermute(give, "tp", [(i, i ^ 1) for i in range(n_tp)])
    far = (keep[:part] + got[:part].astype(jnp.float32)).astype(jnp.bfloat16)
    near = keep[part:] + got[part:].astype(jnp.float32)
    crossed = lax.ppermute(far, "tp", [(i, i ^ 2) for i in range(n_tp)])
    return (near + crossed.astype(jnp.float32)).astype(jnp.bfloat16)


def solution(mesh):
    n, n_tp = mesh.shape["cp"], mesh.shape["tp"]

    def local(queries, keys, values, doc_blocks, block_order, out_weight):
        args = (queries, keys, values, doc_blocks, block_order, out_weight)
        if n == 8 and n_tp == 4 and queries.shape[0] == BLOCK_TOKENS:
            return blockwise(n, n_tp, *args)
        return general(*args)

    placed = (P("cp", "tp"), P("cp", "tp"), P("cp", "tp"), P(), P(), P("tp", None))
    return jax.shard_map(
        local, mesh=mesh, in_specs=placed, out_specs=P(("cp", "tp"), None), check_vma=False
    )
```

```python
import functools

import jax
import jax.numpy as jnp
from jax import lax
from jax.experimental import pallas as pl
from jax.experimental.pallas import tpu as pltpu
from jax.sharding import PartitionSpec as P


HEAD_SIZE = 128
BLOCK_TOKENS = 128
MASKED = -1e30
SCALE = HEAD_SIZE**-0.5 * 1.4426950408889634


def lookup(entries, indices):
    matches = indices[:, None] == jnp.arange(entries.shape[0], dtype=jnp.int32)[None, :]
    return jnp.sum(jnp.where(matches, entries[None, :], 0), axis=1)


def locate(row_ids, block_order, doc_ends):
    seq_block = lookup(block_order, row_ids // BLOCK_TOKENS)
    position = seq_block * BLOCK_TOKENS + row_ids % BLOCK_TOKENS
    doc_ids = jnp.sum((seq_block[:, None] >= doc_ends[None, :]).astype(jnp.int32), axis=1)
    return (position, doc_ids)


def attend(online, key_rows, value_rows, key_pos, key_doc, query_rows, query_pos, query_doc):
    allowed = (query_doc[:, None] == key_doc[None, :]) & (key_pos[None, :] <= query_pos[:, None])
    running_max, weight_sum, weighted = online
    scores = jnp.einsum(
        "qhgd,khd->hgqk", query_rows, key_rows, preferred_element_type=jnp.float32
    ) * HEAD_SIZE ** (-0.5)
    scores = jnp.where(allowed, scores, MASKED)
    new_max = jnp.maximum(running_max, jnp.max(scores, axis=-1))
    weights = jnp.where(allowed, jnp.exp(scores - new_max[..., None]), 0.0)
    factor = jnp.exp(running_max - new_max)
    weight_sum = weight_sum * factor + jnp.sum(weights, axis=-1)
    weighted = weighted * factor[..., None] + jnp.einsum(
        "hgqk,khd->hgqd",
        weights.astype(jnp.bfloat16),
        value_rows,
        preferred_element_type=jnp.float32,
    )
    return (new_max, weight_sum, weighted)


def sweep_keys(
    online, key_part, value_part, block_order, doc_ends, query_rows, query_pos, query_doc
):
    length = key_part.shape[0]
    heads_kv = key_part.shape[1] // HEAD_SIZE
    block_rows = 4 * BLOCK_TOKENS
    token_blocks = length // block_rows
    key_pos, key_doc = locate(jnp.arange(length, dtype=jnp.int32), block_order, doc_ends)

    def scan_step(status, pieces_now):
        return attend(status, *pieces_now, query_rows, query_pos, query_doc), None

    online, _ = lax.scan(
        scan_step,
        online,
        (
            key_part.reshape(token_blocks, block_rows, heads_kv, HEAD_SIZE),
            value_part.reshape(token_blocks, block_rows, heads_kv, HEAD_SIZE),
            key_pos.reshape(token_blocks, block_rows),
            key_doc.reshape(token_blocks, block_rows),
        ),
    )
    return online


def general(queries, keys, values, doc_blocks, block_order, out_weight):
    rows_dev = queries.shape[0]
    heads_kv = keys.shape[1] // HEAD_SIZE
    group_size = queries.shape[1] // keys.shape[1]
    doc_ends = jnp.cumsum(doc_blocks)
    first_row = lax.axis_index("cp") * rows_dev
    query_pos, query_doc = locate(
        first_row + jnp.arange(rows_dev, dtype=jnp.int32), block_order, doc_ends
    )
    query_rows = queries.reshape(rows_dev, heads_kv, group_size, HEAD_SIZE)
    starting_state = (
        jnp.full((heads_kv, group_size, rows_dev), MASKED, jnp.float32),
        jnp.zeros((heads_kv, group_size, rows_dev), jnp.float32),
        jnp.zeros((heads_kv, group_size, rows_dev, HEAD_SIZE), jnp.float32),
    )
    whole_keys = lax.all_gather(keys, "cp", axis=0, tiled=True)
    whole_values = lax.all_gather(values, "cp", axis=0, tiled=True)
    _, weight_sum, weighted = sweep_keys(
        starting_state, whole_keys, whole_values, block_order, doc_ends,
        query_rows, query_pos, query_doc,
    )
    attended = (
        jnp.transpose(weighted / weight_sum[..., None], (2, 0, 1, 3))
        .reshape(rows_dev, -1)
        .astype(jnp.bfloat16)
    )
    return lax.psum_scatter(
        jnp.dot(attended, out_weight, preferred_element_type=jnp.float32).astype(jnp.bfloat16),
        "tp",
        scatter_dimension=0,
        tiled=True,
    )


def spread(x, width):
    return jnp.concatenate([x] * (width // x.shape[1]), 1)


def online(top_ref, sum_ref, at, queries, key_rows, value_rows, bias, fresh=False):
    scores = lax.dot_general(
        queries, key_rows, (((1,), (1,)), ((), ())), preferred_element_type=jnp.float32
    )
    if bias is not None:
        scores = scores + bias
    top = jnp.broadcast_to(jnp.max(scores, axis=1, keepdims=True), (scores.shape[0], HEAD_SIZE))
    if not fresh:
        before = top_ref[at, :]
        top = jnp.maximum(top, before)
    weights = jnp.exp2((scores - spread(top, scores.shape[1])) * SCALE).astype(jnp.bfloat16)
    sums = jnp.dot(weights, value_rows, preferred_element_type=jnp.float32)
    if not fresh:
        sums = sums + sum_ref[at, :] * spread(jnp.exp2((before - top) * SCALE), sums.shape[1])
    top_ref[at, :] = top
    sum_ref[at, :] = sums


def sweep(qr_ref, top_ref, sum_ref, kvs, bias, fresh=False, pieces=2):
    heads_kv = kvs[0].shape[1] // HEAD_SIZE
    height = qr_ref.shape[0] // heads_kv
    for g in range(heads_kv):
        cols = slice(g * HEAD_SIZE, (g + 1) * HEAD_SIZE)
        key_rows = jnp.concatenate([ref[:BLOCK_TOKENS, cols] for ref in kvs], 0)
        value_rows = jnp.concatenate([ref[BLOCK_TOKENS:, cols] for ref in kvs], 0)
        value_rows = jnp.concatenate([value_rows, jnp.ones_like(value_rows)], 1)
        for i in range(pieces):
            at = pl.ds(g * height + i * (height // pieces), height // pieces)
            online(top_ref, sum_ref, at, qr_ref[at, :], key_rows, value_rows, bias, fresh)


def start_all(copies):
    for copy in copies:
        copy.start()
    return copies


def wait_all(copies):
    for copy in copies:
        copy.wait()


def load_rows(src, first, out, sems):
    pieces = sems.shape[0]
    rows = out.shape[0] // pieces
    return start_all([
        pltpu.make_async_copy(
            src.at[pl.ds(first + i * rows, rows)], out.at[pl.ds(i * rows, rows)], sems.at[i])
        for i in range(pieces)
    ])


def begin(n_tp, order_hbm, docs_hbm, q_hbm, w_hbm, kv_ref, qr_ref, seen_ref, top_ref, sum_ref, w_ref,
          q_ref, order_ref, docs_ref, sems, w_sems):
    copies = start_all([
        pltpu.make_async_copy(src, dst, sems.at[i])
        for i, (src, dst) in enumerate(
            ((order_hbm, order_ref), (docs_hbm, docs_ref), (q_hbm, q_ref)))
    ])
    loads = load_rows(w_hbm, 0, w_ref, w_sems)
    wait_all(copies)
    n_blocks, n_docs = order_ref.shape[0], docs_ref.shape[0]
    rows, width = q_ref.shape
    part = rows // n_tp
    me, core = lax.axis_index("cp"), lax.axis_index("tp")
    ends = []
    for d in range(n_docs):
        ends.append(docs_ref[d] + (ends[-1] if ends else 0))

    def document(seq):
        return sum((seq >= end).astype(jnp.int32) for end in ends)

    own_seq = order_ref[me]
    own_doc = document(own_seq)
    for s in range(n_blocks):
        seq = order_ref[me ^ s]
        seen = (document(seq) == own_doc) & (seq < own_seq)
        seen_ref[s : s + 1, :] = jnp.full((1, HEAD_SIZE), seen.astype(jnp.int32), jnp.int32)

    targets = [core ^ f for f in (3, 1, 2, 0)]
    for h in range(width // HEAD_SIZE):
        for p, target in enumerate(targets):
            qr_ref[h * rows + p * part : h * rows + (p + 1) * part, :] = q_ref[
                pl.ds(pl.multiple_of(target * part, part), part),
                h * HEAD_SIZE : (h + 1) * HEAD_SIZE]
    key_at = lax.broadcasted_iota(jnp.int32, (part, BLOCK_TOKENS), 1)
    row_at = lax.broadcasted_iota(jnp.int32, (part, BLOCK_TOKENS), 0)
    bias = jnp.concatenate(
        [jnp.where(key_at <= row_at + target * part, 0.0, MASKED) for target in targets], 0)
    heads = width // kv_ref.shape[1]
    sweep(qr_ref, top_ref, sum_ref, [kv_ref], jnp.concatenate([bias] * (heads // 2), 0), fresh=True)
    wait_all(loads)


def seen_blocks(slots, seen_hbm, seen_smem, sem, qr_ref, top_ref, sum_ref, kv_refs, kv_ref):
    wait_all(start_all([pltpu.make_async_copy(seen_hbm, seen_smem, sem)]))
    used = jnp.int32(0)
    for s, ref in zip(slots, kv_refs):
        wanted = seen_smem[s, 0]

        @pl.when(wanted == 1)
        def _(ref=ref, used=used):
            kv_ref[used] = ref[...]

        used = used + wanted
    for first in range(0, kv_ref.shape[0], 2):
        for count in (1, 2):
            if first + count > kv_ref.shape[0]:
                continue

            @pl.when((used >= first + 2) if count == 2 else (used == first + 1))
            def _(first=first, count=count):
                sweep(qr_ref, top_ref, sum_ref, [kv_ref.at[first + i] for i in range(count)], None)


def more(slots, seen_ref, w_hbm, qr_ref, top_in, sum_in, *refs):
    kv_refs, (top_ref, sum_ref, w_ref, kv_ref, seen_smem, sem, w_sems) = (
        refs[: len(slots)], refs[len(slots) :])
    loads = load_rows(w_hbm, w_ref.shape[0], w_ref, w_sems)
    seen_blocks(slots, seen_ref, seen_smem, sem, qr_ref, top_ref, sum_ref, kv_refs, kv_ref)
    wait_all(loads)


def finish(slots, chunk, seen_ref, qr_ref, top_in, sum_in, *refs):
    kv_refs, (w0_ref, w1_ref, top_ref, sum_ref, give_ref, keep_ref, att_ref, kv_ref, seen_smem, sem) = (
        refs[: len(slots)], refs[len(slots) :])
    seen_blocks(slots, seen_ref, seen_smem, sem, qr_ref, top_ref, sum_ref, kv_refs, kv_ref)
    rows, width = att_ref.shape
    for h in range(width // HEAD_SIZE):
        at = slice(h * rows, (h + 1) * rows)
        att_ref[:, h * HEAD_SIZE : (h + 1) * HEAD_SIZE] = (
            sum_ref[at, :HEAD_SIZE] / sum_ref[at, HEAD_SIZE:]
        ).astype(jnp.bfloat16)
    depth = w0_ref.shape[0]
    for j in range(w0_ref.shape[1] // chunk):
        cols = slice(j * chunk, (j + 1) * chunk)
        product = jnp.dot(att_ref[:, :depth], w0_ref[:, cols], preferred_element_type=jnp.float32)
        product += jnp.dot(att_ref[:, depth:], w1_ref[:, cols], preferred_element_type=jnp.float32)
        give_ref[:, cols] = product[: rows // 2].astype(jnp.bfloat16)
        keep_ref[:, cols] = product[rows // 2 :]


def in_hbm(x):
    return pltpu.with_memory_space_constraint(x, pltpu.HBM)


def in_vmem(x):
    return pltpu.with_memory_space_constraint(x, pltpu.VMEM)


HBM = pl.BlockSpec(memory_space=pltpu.HBM)
VMEM = pl.BlockSpec(memory_space=pltpu.VMEM)


def kernel(body, inputs, outs, scratch=(), flops=0, aliases={}, limit=16):
    return pl.pallas_call(
        body,
        out_shape=tuple(pltpu.VMEM(shape, dtype) for shape, dtype in outs),
        in_specs=[HBM if where == "hbm" else VMEM for where, _ in inputs],
        out_specs=(VMEM,) * len(outs),
        scratch_shapes=list(scratch),
        input_output_aliases=aliases,
        compiler_params=pltpu.CompilerParams(vmem_limit_bytes=limit * 1024 * 1024),
        cost_estimate=pl.CostEstimate(flops=flops, bytes_accessed=0, transcendentals=0),
    )(*[in_hbm(x) if where == "hbm" else in_vmem(x) for where, x in inputs])


def stack_kernel(k_hbm, v_hbm, out_ref, sems):
    rows = k_hbm.shape[0]
    copies = [
        pltpu.make_async_copy(k_hbm, out_ref.at[:rows], sems.at[0]),
        pltpu.make_async_copy(v_hbm, out_ref.at[rows:], sems.at[1]),
    ]
    for copy in copies:
        copy.start()
    for copy in copies:
        copy.wait()


PLAN = ((4, 0, 4), (2, 0, 2), (1, 0, 1), (7, 0, 7), (3, 2, 1), (6, 4, 2), (5, 4, 1))


def blockwise(n, n_tp, queries, keys, values, doc_blocks, block_order, out_weight):
    rows, width = queries.shape
    heads = width // HEAD_SIZE
    out_width = out_weight.shape[1]
    bf16, f32 = jnp.bfloat16, jnp.float32

    def swap(block, s):
        return lax.ppermute(block, "cp", [(i, i ^ s) for i in range(n)])

    (kv,) = kernel(
        stack_kernel, [("hbm", keys), ("hbm", values)],
        [((2 * rows, keys.shape[1]), bf16)], [pltpu.SemaphoreType.DMA((2,))])
    got = {0: kv}
    for s, via, hop in PLAN:
        got[s] = swap(got[via], hop)

    states = [((heads * rows, HEAD_SIZE), f32), ((heads * rows, 2 * HEAD_SIZE), f32)]
    half_weight = ((width // 2, out_width), bf16)
    dma = pltpu.SemaphoreType.DMA
    qr, seen, top, sums, weight0 = kernel(
        functools.partial(begin, n_tp),
        [("hbm", block_order), ("hbm", doc_blocks), ("hbm", queries), ("hbm", out_weight), ("vmem", kv)],
        [((heads * rows, HEAD_SIZE), bf16), ((n, HEAD_SIZE), jnp.int32)] + states + [half_weight],
        [pltpu.VMEM((rows, width), bf16), pltpu.SMEM(block_order.shape, jnp.int32),
         pltpu.SMEM(doc_blocks.shape, jnp.int32), dma((3,)), dma((8,))],
        flops=4 * 10**9, limit=8)
    small = [pltpu.SMEM((n, HEAD_SIZE), jnp.int32), dma(())]

    def held(slots):
        return pltpu.VMEM((min(len(slots), n // 2 - 1),) + kv.shape, bf16)

    slots = (1, 2, 4)
    top, sums, weight1 = kernel(
        functools.partial(more, slots),
        [("vmem", seen), ("hbm", out_weight)]
        + [("vmem", x) for x in (qr, top, sums, *(got[s] for s in slots))],
        states + [half_weight], [held(slots)] + small + [dma((8,))],
        flops=4 * 10**9, aliases={3: 0, 4: 1}, limit=8)
    slots = (3, 7, 6, 5)
    _, _, give, keep = kernel(
        functools.partial(finish, slots, 512),
        [("vmem", x) for x in (seen, qr, top, sums, *(got[s] for s in slots), weight0, weight1)],
        states + [((rows // 2, out_width), bf16), ((rows // 2, out_width), f32)],
        [pltpu.VMEM((rows, width), bf16), held(slots)] + small,
        flops=2 * rows * width * out_width, aliases={2: 0, 3: 1}, limit=8)
    part = rows // n_tp
    got = lax.ppermute(give, "tp", [(i, i ^ 1) for i in range(n_tp)])
    far = (keep[:part] + got[:part].astype(f32)).astype(bf16)
    near = keep[part:] + got[part:].astype(f32)
    crossed = lax.ppermute(far, "tp", [(i, i ^ 2) for i in range(n_tp)])
    return (near + crossed.astype(f32)).astype(bf16)


def solution(mesh):
    n, n_tp = mesh.shape["cp"], mesh.shape["tp"]

    def local(queries, keys, values, doc_blocks, block_order, out_weight):
        args = (queries, keys, values, doc_blocks, block_order, out_weight)
        if n == 8 and n_tp == 4:
            return blockwise(n, n_tp, *args)
        return general(*args)

    placed = (P("cp", "tp"), P("cp", "tp"), P("cp", "tp"), P(), P(), P("tp", None))
    return jax.shard_map(
        local, mesh=mesh, in_specs=placed, out_specs=P(("cp", "tp"), None), check_vma=False
    )
```

```python
import functools

import jax
import jax.numpy as jnp
from jax import lax
from jax.experimental import pallas as pl
from jax.experimental.pallas import tpu as pltpu
from jax.sharding import PartitionSpec as P


HEAD_SIZE = 128
BLOCK_TOKENS = 128
MASKED = -1e30
SCALE = HEAD_SIZE**-0.5 * 1.4426950408889634


def lookup(entries, indices):
    matches = indices[:, None] == jnp.arange(entries.shape[0], dtype=jnp.int32)[None, :]
    return jnp.sum(jnp.where(matches, entries[None, :], 0), axis=1)


def locate(row_ids, block_order, doc_ends):
    seq_block = lookup(block_order, row_ids // BLOCK_TOKENS)
    position = seq_block * BLOCK_TOKENS + row_ids % BLOCK_TOKENS
    doc_ids = jnp.sum((seq_block[:, None] >= doc_ends[None, :]).astype(jnp.int32), axis=1)
    return (position, doc_ids)


def attend(online, key_rows, value_rows, key_pos, key_doc, query_rows, query_pos, query_doc):
    allowed = (query_doc[:, None] == key_doc[None, :]) & (key_pos[None, :] <= query_pos[:, None])
    running_max, weight_sum, weighted = online
    scores = jnp.einsum(
        "qhgd,khd->hgqk", query_rows, key_rows, preferred_element_type=jnp.float32
    ) * HEAD_SIZE ** (-0.5)
    scores = jnp.where(allowed, scores, MASKED)
    new_max = jnp.maximum(running_max, jnp.max(scores, axis=-1))
    weights = jnp.where(allowed, jnp.exp(scores - new_max[..., None]), 0.0)
    factor = jnp.exp(running_max - new_max)
    weight_sum = weight_sum * factor + jnp.sum(weights, axis=-1)
    weighted = weighted * factor[..., None] + jnp.einsum(
        "hgqk,khd->hgqd",
        weights.astype(jnp.bfloat16),
        value_rows,
        preferred_element_type=jnp.float32,
    )
    return (new_max, weight_sum, weighted)


def sweep_keys(
    online, key_part, value_part, block_order, doc_ends, query_rows, query_pos, query_doc
):
    length = key_part.shape[0]
    heads_kv = key_part.shape[1] // HEAD_SIZE
    block_rows = 4 * BLOCK_TOKENS
    token_blocks = length // block_rows
    key_pos, key_doc = locate(jnp.arange(length, dtype=jnp.int32), block_order, doc_ends)

    def scan_step(status, pieces_now):
        return attend(status, *pieces_now, query_rows, query_pos, query_doc), None

    online, _ = lax.scan(
        scan_step,
        online,
        (
            key_part.reshape(token_blocks, block_rows, heads_kv, HEAD_SIZE),
            value_part.reshape(token_blocks, block_rows, heads_kv, HEAD_SIZE),
            key_pos.reshape(token_blocks, block_rows),
            key_doc.reshape(token_blocks, block_rows),
        ),
    )
    return online


def general(queries, keys, values, doc_blocks, block_order, out_weight):
    rows_dev = queries.shape[0]
    heads_kv = keys.shape[1] // HEAD_SIZE
    group_size = queries.shape[1] // keys.shape[1]
    doc_ends = jnp.cumsum(doc_blocks)
    first_row = lax.axis_index("cp") * rows_dev
    query_pos, query_doc = locate(
        first_row + jnp.arange(rows_dev, dtype=jnp.int32), block_order, doc_ends
    )
    query_rows = queries.reshape(rows_dev, heads_kv, group_size, HEAD_SIZE)
    starting_state = (
        jnp.full((heads_kv, group_size, rows_dev), MASKED, jnp.float32),
        jnp.zeros((heads_kv, group_size, rows_dev), jnp.float32),
        jnp.zeros((heads_kv, group_size, rows_dev, HEAD_SIZE), jnp.float32),
    )
    whole_keys = lax.all_gather(keys, "cp", axis=0, tiled=True)
    whole_values = lax.all_gather(values, "cp", axis=0, tiled=True)
    _, weight_sum, weighted = sweep_keys(
        starting_state, whole_keys, whole_values, block_order, doc_ends,
        query_rows, query_pos, query_doc,
    )
    attended = (
        jnp.transpose(weighted / weight_sum[..., None], (2, 0, 1, 3))
        .reshape(rows_dev, -1)
        .astype(jnp.bfloat16)
    )
    return lax.psum_scatter(
        jnp.dot(attended, out_weight, preferred_element_type=jnp.float32).astype(jnp.bfloat16),
        "tp",
        scatter_dimension=0,
        tiled=True,
    )


def spread(x, width):
    return jnp.concatenate([x] * (width // x.shape[1]), 1)


def online(top_ref, sum_ref, at, queries, key_rows, value_rows, bias, fresh=False):
    scores = lax.dot_general(
        queries, key_rows, (((1,), (1,)), ((), ())), preferred_element_type=jnp.float32
    )
    if bias is not None:
        scores = scores + bias
    top = jnp.broadcast_to(jnp.max(scores, axis=1, keepdims=True), (scores.shape[0], HEAD_SIZE))
    if not fresh:
        before = top_ref[at, :]
        top = jnp.maximum(top, before)
    weights = jnp.exp2((scores - spread(top, scores.shape[1])) * SCALE).astype(jnp.bfloat16)
    sums = jnp.dot(weights, value_rows, preferred_element_type=jnp.float32)
    if not fresh:
        sums = sums + sum_ref[at, :] * spread(jnp.exp2((before - top) * SCALE), sums.shape[1])
    top_ref[at, :] = top
    sum_ref[at, :] = sums


def sweep(qr_ref, top_ref, sum_ref, kvs, bias, fresh=False, pieces=2):
    heads_kv = kvs[0].shape[1] // HEAD_SIZE
    height = qr_ref.shape[0] // heads_kv
    for g in range(heads_kv):
        cols = slice(g * HEAD_SIZE, (g + 1) * HEAD_SIZE)
        key_rows = jnp.concatenate([ref[:BLOCK_TOKENS, cols] for ref in kvs], 0)
        value_rows = jnp.concatenate([ref[BLOCK_TOKENS:, cols] for ref in kvs], 0)
        value_rows = jnp.concatenate([value_rows, jnp.ones_like(value_rows)], 1)
        for i in range(pieces):
            at = pl.ds(g * height + i * (height // pieces), height // pieces)
            online(top_ref, sum_ref, at, qr_ref[at, :], key_rows, value_rows, bias, fresh)


def start_all(copies):
    for copy in copies:
        copy.start()
    return copies


def wait_all(copies):
    for copy in copies:
        copy.wait()


def load_rows(src, first, out, sems):
    pieces = sems.shape[0]
    rows = out.shape[0] // pieces
    return start_all([
        pltpu.make_async_copy(
            src.at[pl.ds(first + i * rows, rows)], out.at[pl.ds(i * rows, rows)], sems.at[i])
        for i in range(pieces)
    ])


def begin(n_tp, order_hbm, docs_hbm, q_hbm, w_hbm, kv_ref, qr_ref, seen_ref, top_ref, sum_ref, w_ref,
          q_ref, order_ref, docs_ref, sems, w_sems):
    copies = start_all([
        pltpu.make_async_copy(src, dst, sems.at[i])
        for i, (src, dst) in enumerate(
            ((order_hbm, order_ref), (docs_hbm, docs_ref), (q_hbm, q_ref)))
    ])
    loads = load_rows(w_hbm, 0, w_ref, w_sems)
    wait_all(copies)
    n_blocks, n_docs = order_ref.shape[0], docs_ref.shape[0]
    rows, width = q_ref.shape
    part = rows // n_tp
    me, core = lax.axis_index("cp"), lax.axis_index("tp")
    ends = []
    for d in range(n_docs):
        ends.append(docs_ref[d] + (ends[-1] if ends else 0))

    def document(seq):
        return sum((seq >= end).astype(jnp.int32) for end in ends)

    own_seq = order_ref[me]
    own_doc = document(own_seq)
    for s in range(n_blocks):
        seq = order_ref[me ^ s]
        seen = (document(seq) == own_doc) & (seq < own_seq)
        seen_ref[s : s + 1, :] = jnp.full((1, HEAD_SIZE), seen.astype(jnp.int32), jnp.int32)

    targets = [core ^ f for f in (3, 1, 2, 0)]
    for h in range(width // HEAD_SIZE):
        for p, target in enumerate(targets):
            qr_ref[h * rows + p * part : h * rows + (p + 1) * part, :] = q_ref[
                pl.ds(pl.multiple_of(target * part, part), part),
                h * HEAD_SIZE : (h + 1) * HEAD_SIZE]
    key_at = lax.broadcasted_iota(jnp.int32, (part, BLOCK_TOKENS), 1)
    row_at = lax.broadcasted_iota(jnp.int32, (part, BLOCK_TOKENS), 0)
    bias = jnp.concatenate(
        [jnp.where(key_at <= row_at + target * part, 0.0, MASKED) for target in targets], 0)
    heads = width // kv_ref.shape[1]
    sweep(qr_ref, top_ref, sum_ref, [kv_ref], jnp.concatenate([bias] * (heads // 2), 0), fresh=True)
    wait_all(loads)


def seen_blocks(slots, seen_hbm, seen_smem, sem, qr_ref, top_ref, sum_ref, kv_refs, kv_ref):
    wait_all(start_all([pltpu.make_async_copy(seen_hbm, seen_smem, sem)]))
    used = jnp.int32(0)
    for s, ref in zip(slots, kv_refs):
        wanted = seen_smem[s, 0]

        @pl.when(wanted == 1)
        def _(ref=ref, used=used):
            kv_ref[used] = ref[...]

        used = used + wanted
    for first in range(0, kv_ref.shape[0], 2):
        for count in (1, 2):
            if first + count > kv_ref.shape[0]:
                continue

            @pl.when((used >= first + 2) if count == 2 else (used == first + 1))
            def _(first=first, count=count):
                sweep(qr_ref, top_ref, sum_ref, [kv_ref.at[first + i] for i in range(count)], None)


def more(slots, seen_ref, w_hbm, qr_ref, top_in, sum_in, *refs):
    kv_refs, (top_ref, sum_ref, w_ref, kv_ref, seen_smem, sem, w_sems) = (
        refs[: len(slots)], refs[len(slots) :])
    loads = load_rows(w_hbm, w_ref.shape[0], w_ref, w_sems)
    seen_blocks(slots, seen_ref, seen_smem, sem, qr_ref, top_ref, sum_ref, kv_refs, kv_ref)
    wait_all(loads)


def again(slots, seen_ref, qr_ref, top_in, sum_in, *refs):
    kv_refs, (top_ref, sum_ref, kv_ref, seen_smem, sem) = refs[: len(slots)], refs[len(slots) :]
    seen_blocks(slots, seen_ref, seen_smem, sem, qr_ref, top_ref, sum_ref, kv_refs, kv_ref)


def project(att_ref, w_refs, first, chunk, give_ref, keep_ref):
    half = att_ref.shape[0] // 2
    for j in range(give_ref.shape[1] // chunk):
        product, depth = None, 0
        for w_ref in w_refs:
            term = jnp.dot(
                att_ref[:, depth : depth + w_ref.shape[0]],
                w_ref[:, first + j * chunk : first + (j + 1) * chunk],
                preferred_element_type=jnp.float32)
            product = term if product is None else product + term
            depth += w_ref.shape[0]
        give_ref[:, j * chunk : (j + 1) * chunk] = product[:half].astype(jnp.bfloat16)
        keep_ref[:, j * chunk : (j + 1) * chunk] = product[half:]


def finish(slots, chunk, seen_ref, qr_ref, top_in, sum_in, *refs):
    kv_refs, (w0_ref, w1_ref, top_ref, sum_ref, att_ref, give_ref, keep_ref, kv_ref, seen_smem, sem) = (
        refs[: len(slots)], refs[len(slots) :])
    seen_blocks(slots, seen_ref, seen_smem, sem, qr_ref, top_ref, sum_ref, kv_refs, kv_ref)
    rows, width = att_ref.shape
    for h in range(width // HEAD_SIZE):
        at = slice(h * rows, (h + 1) * rows)
        att_ref[:, h * HEAD_SIZE : (h + 1) * HEAD_SIZE] = (
            sum_ref[at, :HEAD_SIZE] / sum_ref[at, HEAD_SIZE:]
        ).astype(jnp.bfloat16)
    project(att_ref, (w0_ref, w1_ref), 0, chunk, give_ref, keep_ref)


def rest(chunk, att_ref, w0_ref, w1_ref, give_ref, keep_ref):
    project(att_ref, (w0_ref, w1_ref), w0_ref.shape[1] - give_ref.shape[1], chunk, give_ref, keep_ref)


def in_hbm(x):
    return pltpu.with_memory_space_constraint(x, pltpu.HBM)


def in_vmem(x):
    return pltpu.with_memory_space_constraint(x, pltpu.VMEM)


HBM = pl.BlockSpec(memory_space=pltpu.HBM)
VMEM = pl.BlockSpec(memory_space=pltpu.VMEM)


def kernel(body, inputs, outs, scratch=(), flops=0, aliases={}, limit=16):
    return pl.pallas_call(
        body,
        out_shape=tuple(pltpu.VMEM(shape, dtype) for shape, dtype in outs),
        in_specs=[HBM if where == "hbm" else VMEM for where, _ in inputs],
        out_specs=(VMEM,) * len(outs),
        scratch_shapes=list(scratch),
        input_output_aliases=aliases,
        compiler_params=pltpu.CompilerParams(vmem_limit_bytes=limit * 1024 * 1024),
        cost_estimate=pl.CostEstimate(flops=flops, bytes_accessed=0, transcendentals=0),
    )(*[in_hbm(x) if where == "hbm" else in_vmem(x) for where, x in inputs])


def stack_kernel(k_hbm, v_hbm, out_ref, sems):
    rows = k_hbm.shape[0]
    copies = [
        pltpu.make_async_copy(k_hbm, out_ref.at[:rows], sems.at[0]),
        pltpu.make_async_copy(v_hbm, out_ref.at[rows:], sems.at[1]),
    ]
    for copy in copies:
        copy.start()
    for copy in copies:
        copy.wait()


PLAN = ((4, 0, 4), (2, 0, 2), (1, 0, 1), (7, 0, 7), (3, 2, 1), (6, 4, 2), (5, 4, 1))


def blockwise(n, n_tp, queries, keys, values, doc_blocks, block_order, out_weight):
    rows, width = queries.shape
    heads = width // HEAD_SIZE
    out_width = out_weight.shape[1]
    bf16, f32 = jnp.bfloat16, jnp.float32

    def swap(block, s):
        return lax.ppermute(block, "cp", [(i, i ^ s) for i in range(n)])

    (kv,) = kernel(
        stack_kernel, [("hbm", keys), ("hbm", values)],
        [((2 * rows, keys.shape[1]), bf16)], [pltpu.SemaphoreType.DMA((2,))])
    got = {0: kv}
    for s, via, hop in PLAN:
        got[s] = swap(got[via], hop)

    states = [((heads * rows, HEAD_SIZE), f32), ((heads * rows, 2 * HEAD_SIZE), f32)]
    half_weight = ((width // 2, out_width), bf16)
    dma = pltpu.SemaphoreType.DMA
    qr, seen, top, sums, weight0 = kernel(
        functools.partial(begin, n_tp),
        [("hbm", block_order), ("hbm", doc_blocks), ("hbm", queries), ("hbm", out_weight), ("vmem", kv)],
        [((heads * rows, HEAD_SIZE), bf16), ((n, HEAD_SIZE), jnp.int32)] + states + [half_weight],
        [pltpu.VMEM((rows, width), bf16), pltpu.SMEM(block_order.shape, jnp.int32),
         pltpu.SMEM(doc_blocks.shape, jnp.int32), dma((3,)), dma((8,))],
        flops=4 * 10**9, limit=8)
    small = [pltpu.SMEM((n, HEAD_SIZE), jnp.int32), dma(())]

    def held(slots):
        return pltpu.VMEM((min(len(slots), n // 2 - 1),) + kv.shape, bf16)

    slots = (1, 2, 4)
    top, sums, weight1 = kernel(
        functools.partial(more, slots),
        [("vmem", seen), ("hbm", out_weight)]
        + [("vmem", x) for x in (qr, top, sums, *(got[s] for s in slots))],
        states + [half_weight], [held(slots)] + small + [dma((8,))],
        flops=4 * 10**9, aliases={3: 0, 4: 1}, limit=8)
    slots = (3, 7)
    top, sums = kernel(
        functools.partial(again, slots),
        [("vmem", x) for x in (seen, qr, top, sums, *(got[s] for s in slots))],
        states, [held(slots)] + small, flops=10**9, aliases={2: 0, 3: 1}, limit=8)
    slots = (6, 5)
    part, chunk, half = rows // n_tp, 512, out_width // 2
    shares = [((rows // 2, half), bf16), ((rows // 2, half), f32)]
    _, _, att, give0, keep0 = kernel(
        functools.partial(finish, slots, chunk),
        [("vmem", x) for x in (seen, qr, top, sums, *(got[s] for s in slots), weight0, weight1)],
        states + [((rows, width), bf16)] + shares, [held(slots)] + small,
        flops=rows * width * out_width, aliases={2: 0, 3: 1}, limit=8)

    def across(x, hop):
        return lax.ppermute(x, "tp", [(i, i ^ hop) for i in range(n_tp)])

    got0 = across(give0, 1)
    give1, keep1 = kernel(
        functools.partial(rest, chunk), [("vmem", x) for x in (att, weight0, weight1)],
        shares, flops=rows * width * out_width, limit=8)
    got1 = across(give1, 1)
    ends = []
    for keep, other in ((keep0, got0), (keep1, got1)):
        far = (keep[:part] + other[:part].astype(f32)).astype(bf16)
        crossed = across(far, 2)
        ends.append((keep[part:] + other[part:].astype(f32) + crossed.astype(f32)).astype(bf16))
    return jnp.concatenate(ends, 1)


def solution(mesh):
    n, n_tp = mesh.shape["cp"], mesh.shape["tp"]

    def local(queries, keys, values, doc_blocks, block_order, out_weight):
        args = (queries, keys, values, doc_blocks, block_order, out_weight)
        if n == 8 and n_tp == 4:
            return blockwise(n, n_tp, *args)
        return general(*args)

    placed = (P("cp", "tp"), P("cp", "tp"), P("cp", "tp"), P(), P(), P("tp", None))
    return jax.shard_map(
        local, mesh=mesh, in_specs=placed, out_specs=P(("cp", "tp"), None), check_vma=False
    )
```

```python
import functools

import jax
import jax.numpy as jnp
from jax import lax
from jax.experimental import pallas as pl
from jax.experimental.pallas import tpu as pltpu
from jax.sharding import PartitionSpec as P


HEAD_SIZE = 128
BLOCK_TOKENS = 128
MASKED = -1e30
SCALE = HEAD_SIZE**-0.5 * 1.4426950408889634


def lookup(entries, indices):
    matches = indices[:, None] == jnp.arange(entries.shape[0], dtype=jnp.int32)[None, :]
    return jnp.sum(jnp.where(matches, entries[None, :], 0), axis=1)


def locate(row_ids, block_order, doc_ends):
    seq_block = lookup(block_order, row_ids // BLOCK_TOKENS)
    position = seq_block * BLOCK_TOKENS + row_ids % BLOCK_TOKENS
    doc_ids = jnp.sum((seq_block[:, None] >= doc_ends[None, :]).astype(jnp.int32), axis=1)
    return (position, doc_ids)


def attend(online, key_rows, value_rows, key_pos, key_doc, query_rows, query_pos, query_doc):
    allowed = (query_doc[:, None] == key_doc[None, :]) & (key_pos[None, :] <= query_pos[:, None])
    running_max, weight_sum, weighted = online
    scores = jnp.einsum(
        "qhgd,khd->hgqk", query_rows, key_rows, preferred_element_type=jnp.float32
    ) * HEAD_SIZE ** (-0.5)
    scores = jnp.where(allowed, scores, MASKED)
    new_max = jnp.maximum(running_max, jnp.max(scores, axis=-1))
    weights = jnp.where(allowed, jnp.exp(scores - new_max[..., None]), 0.0)
    factor = jnp.exp(running_max - new_max)
    weight_sum = weight_sum * factor + jnp.sum(weights, axis=-1)
    weighted = weighted * factor[..., None] + jnp.einsum(
        "hgqk,khd->hgqd",
        weights.astype(jnp.bfloat16),
        value_rows,
        preferred_element_type=jnp.float32,
    )
    return (new_max, weight_sum, weighted)


def sweep_keys(
    online, key_part, value_part, block_order, doc_ends, query_rows, query_pos, query_doc
):
    length = key_part.shape[0]
    heads_kv = key_part.shape[1] // HEAD_SIZE
    block_rows = 4 * BLOCK_TOKENS
    token_blocks = length // block_rows
    key_pos, key_doc = locate(jnp.arange(length, dtype=jnp.int32), block_order, doc_ends)

    def scan_step(status, pieces_now):
        return attend(status, *pieces_now, query_rows, query_pos, query_doc), None

    online, _ = lax.scan(
        scan_step,
        online,
        (
            key_part.reshape(token_blocks, block_rows, heads_kv, HEAD_SIZE),
            value_part.reshape(token_blocks, block_rows, heads_kv, HEAD_SIZE),
            key_pos.reshape(token_blocks, block_rows),
            key_doc.reshape(token_blocks, block_rows),
        ),
    )
    return online


def general(queries, keys, values, doc_blocks, block_order, out_weight):
    rows_dev = queries.shape[0]
    heads_kv = keys.shape[1] // HEAD_SIZE
    group_size = queries.shape[1] // keys.shape[1]
    doc_ends = jnp.cumsum(doc_blocks)
    first_row = lax.axis_index("cp") * rows_dev
    query_pos, query_doc = locate(
        first_row + jnp.arange(rows_dev, dtype=jnp.int32), block_order, doc_ends
    )
    query_rows = queries.reshape(rows_dev, heads_kv, group_size, HEAD_SIZE)
    starting_state = (
        jnp.full((heads_kv, group_size, rows_dev), MASKED, jnp.float32),
        jnp.zeros((heads_kv, group_size, rows_dev), jnp.float32),
        jnp.zeros((heads_kv, group_size, rows_dev, HEAD_SIZE), jnp.float32),
    )
    whole_keys = lax.all_gather(keys, "cp", axis=0, tiled=True)
    whole_values = lax.all_gather(values, "cp", axis=0, tiled=True)
    _, weight_sum, weighted = sweep_keys(
        starting_state, whole_keys, whole_values, block_order, doc_ends,
        query_rows, query_pos, query_doc,
    )
    attended = (
        jnp.transpose(weighted / weight_sum[..., None], (2, 0, 1, 3))
        .reshape(rows_dev, -1)
        .astype(jnp.bfloat16)
    )
    return lax.psum_scatter(
        jnp.dot(attended, out_weight, preferred_element_type=jnp.float32).astype(jnp.bfloat16),
        "tp",
        scatter_dimension=0,
        tiled=True,
    )


def spread(x, width):
    return jnp.concatenate([x] * (width // x.shape[1]), 1)


def online(top_ref, sum_ref, at, queries, key_rows, value_rows, bias, fresh=False):
    scores = lax.dot_general(
        queries, key_rows, (((1,), (1,)), ((), ())), preferred_element_type=jnp.float32
    )
    if bias is not None:
        scores = scores + bias
    top = jnp.broadcast_to(jnp.max(scores, axis=1, keepdims=True), (scores.shape[0], HEAD_SIZE))
    if not fresh:
        before = top_ref[at, :]
        top = jnp.maximum(top, before)
    weights = jnp.exp2((scores - spread(top, scores.shape[1])) * SCALE).astype(jnp.bfloat16)
    sums = jnp.dot(weights, value_rows, preferred_element_type=jnp.float32)
    if not fresh:
        sums = sums + sum_ref[at, :] * spread(jnp.exp2((before - top) * SCALE), sums.shape[1])
    top_ref[at, :] = top
    sum_ref[at, :] = sums


def sweep(qr_ref, top_ref, sum_ref, kvs, bias, fresh=False):
    heads_kv = kvs[0].shape[1] // HEAD_SIZE
    height = qr_ref.shape[0] // heads_kv
    for g in range(heads_kv):
        cols = slice(g * HEAD_SIZE, (g + 1) * HEAD_SIZE)
        key_rows = jnp.concatenate([ref[:BLOCK_TOKENS, cols] for ref in kvs], 0)
        value_rows = jnp.concatenate([ref[BLOCK_TOKENS:, cols] for ref in kvs], 0)
        value_rows = jnp.concatenate([value_rows, jnp.ones_like(value_rows)], 1)
        at = pl.ds(g * height, height)
        online(top_ref, sum_ref, at, qr_ref[at, :], key_rows, value_rows, bias, fresh)


def start_all(copies):
    for copy in copies:
        copy.start()
    return copies


def wait_all(copies):
    for copy in copies:
        copy.wait()


def load_rows(src, first, out, sems):
    pieces = sems.shape[0]
    rows = out.shape[0] // pieces
    return start_all([
        pltpu.make_async_copy(
            src.at[pl.ds(first + i * rows, rows)], out.at[pl.ds(i * rows, rows)], sems.at[i])
        for i in range(pieces)
    ])


def begin(n_tp, order_hbm, docs_hbm, q_hbm, w_hbm, kv_ref, qr_ref, seen_ref, top_ref, sum_ref, w_ref,
          q_ref, order_ref, docs_ref, sems, w_sems):
    copies = start_all([
        pltpu.make_async_copy(src, dst, sems.at[i])
        for i, (src, dst) in enumerate(
            ((order_hbm, order_ref), (docs_hbm, docs_ref), (q_hbm, q_ref)))
    ])
    loads = load_rows(w_hbm, 0, w_ref, w_sems)
    wait_all(copies)
    n_blocks, n_docs = order_ref.shape[0], docs_ref.shape[0]
    rows, width = q_ref.shape
    part = rows // n_tp
    me, core = lax.axis_index("cp"), lax.axis_index("tp")
    ends = []
    for d in range(n_docs):
        ends.append(docs_ref[d] + (ends[-1] if ends else 0))

    def document(seq):
        return sum((seq >= end).astype(jnp.int32) for end in ends)

    own_seq = order_ref[me]
    own_doc = document(own_seq)
    for s in range(n_blocks):
        seq = order_ref[me ^ s]
        seen = (document(seq) == own_doc) & (seq < own_seq)
        seen_ref[s : s + 1, :] = jnp.full((1, HEAD_SIZE), seen.astype(jnp.int32), jnp.int32)

    targets = [core ^ f for f in (3, 1, 2, 0)]
    for h in range(width // HEAD_SIZE):
        for p, target in enumerate(targets):
            qr_ref[h * rows + p * part : h * rows + (p + 1) * part, :] = q_ref[
                pl.ds(pl.multiple_of(target * part, part), part),
                h * HEAD_SIZE : (h + 1) * HEAD_SIZE]
    key_at = lax.broadcasted_iota(jnp.int32, (part, BLOCK_TOKENS), 1)
    row_at = lax.broadcasted_iota(jnp.int32, (part, BLOCK_TOKENS), 0)
    bias = jnp.concatenate(
        [jnp.where(key_at <= row_at + target * part, 0.0, MASKED) for target in targets], 0)
    heads = width // kv_ref.shape[1]
    sweep(qr_ref, top_ref, sum_ref, [kv_ref], jnp.concatenate([bias] * heads, 0), fresh=True)
    wait_all(loads)


def seen_blocks(slots, seen_ref, qr_ref, top_ref, sum_ref, kv_refs, kv_ref):
    used = jnp.int32(0)
    for s, ref in zip(slots, kv_refs):
        wanted = jnp.max(seen_ref[s : s + 1, :])

        @pl.when(wanted == 1)
        def _(ref=ref, used=used):
            kv_ref[used] = ref[...]

        used = used + wanted
    for first in range(0, kv_ref.shape[0], 2):
        for count in (1, 2):
            if first + count > kv_ref.shape[0]:
                continue
            last = first + count == kv_ref.shape[0]

            @pl.when((used >= first + 2) if count == 2 else (used == first + 1))
            def _(first=first, count=count):
                sweep(qr_ref, top_ref, sum_ref, [kv_ref.at[first + i] for i in range(count)], None)


def more(slots, seen_ref, w_hbm, qr_ref, top_in, sum_in, *refs):
    kv_refs, (top_ref, sum_ref, w_ref, kv_ref, w_sems) = (
        refs[: len(slots)], refs[len(slots) :])
    loads = load_rows(w_hbm, w_ref.shape[0], w_ref, w_sems)
    seen_blocks(slots, seen_ref, qr_ref, top_ref, sum_ref, kv_refs, kv_ref)
    wait_all(loads)


def again(slots, seen_ref, qr_ref, top_in, sum_in, *refs):
    kv_refs, (top_ref, sum_ref, kv_ref) = refs[: len(slots)], refs[len(slots) :]
    seen_blocks(slots, seen_ref, qr_ref, top_ref, sum_ref, kv_refs, kv_ref)


def project(att_ref, w_refs, first, chunk, give_ref, keep_ref):
    half = att_ref.shape[0] // 2
    for j in range(give_ref.shape[1] // chunk):
        product, depth = None, 0
        for w_ref in w_refs:
            term = jnp.dot(
                att_ref[:, depth : depth + w_ref.shape[0]],
                w_ref[:, first + j * chunk : first + (j + 1) * chunk],
                preferred_element_type=jnp.float32)
            product = term if product is None else product + term
            depth += w_ref.shape[0]
        give_ref[:, j * chunk : (j + 1) * chunk] = product[:half].astype(jnp.bfloat16)
        keep_ref[:, j * chunk : (j + 1) * chunk] = product[half:]


def finish(slots, chunk, seen_ref, qr_ref, top_in, sum_in, *refs):
    kv_refs, (w0_ref, w1_ref, top_ref, sum_ref, att_ref, give_ref, keep_ref, kv_ref) = (
        refs[: len(slots)], refs[len(slots) :])
    seen_blocks(slots, seen_ref, qr_ref, top_ref, sum_ref, kv_refs, kv_ref)
    rows, width = att_ref.shape
    for h in range(width // HEAD_SIZE):
        at = slice(h * rows, (h + 1) * rows)
        att_ref[:, h * HEAD_SIZE : (h + 1) * HEAD_SIZE] = (
            sum_ref[at, :HEAD_SIZE] * pl.reciprocal(sum_ref[at, HEAD_SIZE:])
        ).astype(jnp.bfloat16)
    project(att_ref, (w0_ref, w1_ref), 0, chunk, give_ref, keep_ref)


def rest(chunk, att_ref, w0_ref, w1_ref, give_ref, keep_ref):
    project(att_ref, (w0_ref, w1_ref), w0_ref.shape[1] - give_ref.shape[1], chunk, give_ref, keep_ref)


def last(at, keep_ref, other_ref, crossed_ref, *refs):
    out_hbm, out_ref, sem = refs[-3:]
    part, width = out_ref.shape
    out_ref[...] = (
        keep_ref[part:] + other_ref[part:].astype(jnp.float32) + crossed_ref[...].astype(jnp.float32)
    ).astype(out_ref.dtype)
    wait_all(start_all([pltpu.make_async_copy(out_ref, out_hbm.at[:, pl.ds(at, width)], sem)]))


def in_hbm(x):
    return pltpu.with_memory_space_constraint(x, pltpu.HBM)


def in_vmem(x):
    return pltpu.with_memory_space_constraint(x, pltpu.VMEM)


HBM = pl.BlockSpec(memory_space=pltpu.HBM)
VMEM = pl.BlockSpec(memory_space=pltpu.VMEM)


def kernel(body, inputs, outs, scratch=(), flops=0, aliases={}, limit=16):
    return pl.pallas_call(
        body,
        out_shape=tuple(pltpu.VMEM(shape, dtype) for shape, dtype in outs),
        in_specs=[HBM if where == "hbm" else VMEM for where, _ in inputs],
        out_specs=(VMEM,) * len(outs),
        scratch_shapes=list(scratch),
        input_output_aliases=aliases,
        compiler_params=pltpu.CompilerParams(vmem_limit_bytes=limit * 1024 * 1024),
        cost_estimate=pl.CostEstimate(flops=flops, bytes_accessed=0, transcendentals=0),
    )(*[in_hbm(x) if where == "hbm" else in_vmem(x) for where, x in inputs])


def stack_kernel(k_hbm, v_hbm, out_ref, sems):
    rows = k_hbm.shape[0]
    copies = [
        pltpu.make_async_copy(k_hbm, out_ref.at[:rows], sems.at[0]),
        pltpu.make_async_copy(v_hbm, out_ref.at[rows:], sems.at[1]),
    ]
    for copy in copies:
        copy.start()
    for copy in copies:
        copy.wait()


PLAN = ((4, 0, 4), (2, 0, 2), (1, 0, 1), (7, 0, 7), (3, 2, 1), (6, 4, 2), (5, 4, 1))


def blockwise(n, n_tp, queries, keys, values, doc_blocks, block_order, out_weight):
    rows, width = queries.shape
    heads = width // HEAD_SIZE
    out_width = out_weight.shape[1]
    bf16, f32 = jnp.bfloat16, jnp.float32

    def swap(block, s):
        return lax.ppermute(block, "cp", [(i, i ^ s) for i in range(n)])

    (kv,) = kernel(
        stack_kernel, [("hbm", keys), ("hbm", values)],
        [((2 * rows, keys.shape[1]), bf16)], [pltpu.SemaphoreType.DMA((2,))])
    got = {0: kv}
    for s, via, hop in PLAN:
        got[s] = swap(got[via], hop)

    states = [((heads * rows, HEAD_SIZE), f32), ((heads * rows, 2 * HEAD_SIZE), f32)]
    half_weight = ((width // 2, out_width), bf16)
    dma = pltpu.SemaphoreType.DMA
    qr, seen, top, sums, weight0 = kernel(
        functools.partial(begin, n_tp),
        [("hbm", block_order), ("hbm", doc_blocks), ("hbm", queries), ("hbm", out_weight), ("vmem", kv)],
        [((heads * rows, HEAD_SIZE), bf16), ((n, HEAD_SIZE), jnp.int32)] + states + [half_weight],
        [pltpu.VMEM((rows, width), bf16), pltpu.SMEM(block_order.shape, jnp.int32),
         pltpu.SMEM(doc_blocks.shape, jnp.int32), dma((3,)), dma((8,))],
        flops=4 * 10**9, limit=8)

    def held(slots):
        return pltpu.VMEM((min(len(slots), n // 2 - 1),) + kv.shape, bf16)

    slots = (1, 2, 4)
    top, sums, weight1 = kernel(
        functools.partial(more, slots),
        [("vmem", seen), ("hbm", out_weight)]
        + [("vmem", x) for x in (qr, top, sums, *(got[s] for s in slots))],
        states + [half_weight], [held(slots), dma((8,))],
        flops=4 * 10**9, aliases={3: 0, 4: 1}, limit=8)
    slots = (3, 7, 6)
    top, sums = kernel(
        functools.partial(again, slots),
        [("vmem", x) for x in (seen, qr, top, sums, *(got[s] for s in slots))],
        states, [held(slots)], flops=10**9, aliases={2: 0, 3: 1}, limit=8)
    slots = (5,)
    part, chunk, half = rows // n_tp, 512, out_width // 2
    shares = [((rows // 2, half), bf16), ((rows // 2, half), f32)]
    _, _, att, give0, keep0 = kernel(
        functools.partial(finish, slots, chunk),
        [("vmem", x) for x in (seen, qr, top, sums, *(got[s] for s in slots), weight0, weight1)],
        states + [((rows, width), bf16)] + shares, [held(slots)],
        flops=rows * width * out_width, aliases={2: 0, 3: 1}, limit=8)

    def across(x, hop):
        return lax.ppermute(x, "tp", [(i, i ^ hop) for i in range(n_tp)])

    got0 = across(give0, 1)
    give1, keep1 = kernel(
        functools.partial(rest, chunk), [("vmem", x) for x in (att, weight0, weight1)],
        shares, flops=rows * width * out_width, limit=8)
    got1 = across(give1, 1)
    crossed = []
    for keep, other in ((keep0, got0), (keep1, got1)):
        far = (keep[:part] + other[:part].astype(f32)).astype(bf16)
        crossed.append(across(far, 2))
    ends = ((keep0, got0, crossed[0]), (keep1, got1, crossed[1]))
    out = ()
    for i, terms in enumerate(ends):
        out = pl.pallas_call(
            functools.partial(last, i * half),
            out_shape=(pltpu.HBM((part, out_width), bf16),),
            in_specs=[VMEM] * 3 + [HBM] * len(out),
            out_specs=(HBM,),
            scratch_shapes=[pltpu.VMEM((part, half), bf16), dma(())],
            input_output_aliases={3: 0} if out else {},
            compiler_params=pltpu.CompilerParams(vmem_limit_bytes=8 * 1024 * 1024),
        )(*map(in_vmem, terms), *out)
    return out[0]


def solution(mesh):
    n, n_tp = mesh.shape["cp"], mesh.shape["tp"]

    def local(queries, keys, values, doc_blocks, block_order, out_weight):
        args = (queries, keys, values, doc_blocks, block_order, out_weight)
        if n == 8 and n_tp == 4:
            return blockwise(n, n_tp, *args)
        return general(*args)

    placed = (P("cp", "tp"), P("cp", "tp"), P("cp", "tp"), P(), P(), P("tp", None))
    return jax.shard_map(
        local, mesh=mesh, in_specs=placed, out_specs=P(("cp", "tp"), None), check_vma=False
    )
```

```python
import functools

import jax
import jax.numpy as jnp
from jax import lax
from jax.experimental import pallas as pl
from jax.experimental.pallas import tpu as pltpu
from jax.sharding import PartitionSpec as P


HEAD_SIZE = 128
BLOCK_TOKENS = 128
MASKED = -1e30
SCALE = HEAD_SIZE**-0.5 * 1.4426950408889634


def lookup(entries, indices):
    matches = indices[:, None] == jnp.arange(entries.shape[0], dtype=jnp.int32)[None, :]
    return jnp.sum(jnp.where(matches, entries[None, :], 0), axis=1)


def locate(row_ids, block_order, doc_ends):
    seq_block = lookup(block_order, row_ids // BLOCK_TOKENS)
    position = seq_block * BLOCK_TOKENS + row_ids % BLOCK_TOKENS
    doc_ids = jnp.sum((seq_block[:, None] >= doc_ends[None, :]).astype(jnp.int32), axis=1)
    return (position, doc_ids)


def attend(online, key_rows, value_rows, key_pos, key_doc, query_rows, query_pos, query_doc):
    allowed = (query_doc[:, None] == key_doc[None, :]) & (key_pos[None, :] <= query_pos[:, None])
    running_max, weight_sum, weighted = online
    scores = jnp.einsum(
        "qhgd,khd->hgqk", query_rows, key_rows, preferred_element_type=jnp.float32
    ) * HEAD_SIZE ** (-0.5)
    scores = jnp.where(allowed, scores, MASKED)
    new_max = jnp.maximum(running_max, jnp.max(scores, axis=-1))
    weights = jnp.where(allowed, jnp.exp(scores - new_max[..., None]), 0.0)
    factor = jnp.exp(running_max - new_max)
    weight_sum = weight_sum * factor + jnp.sum(weights, axis=-1)
    weighted = weighted * factor[..., None] + jnp.einsum(
        "hgqk,khd->hgqd",
        weights.astype(jnp.bfloat16),
        value_rows,
        preferred_element_type=jnp.float32,
    )
    return (new_max, weight_sum, weighted)


def sweep_keys(
    online, key_part, value_part, block_order, doc_ends, query_rows, query_pos, query_doc
):
    length = key_part.shape[0]
    heads_kv = key_part.shape[1] // HEAD_SIZE
    block_rows = 4 * BLOCK_TOKENS
    token_blocks = length // block_rows
    key_pos, key_doc = locate(jnp.arange(length, dtype=jnp.int32), block_order, doc_ends)

    def scan_step(status, pieces_now):
        return attend(status, *pieces_now, query_rows, query_pos, query_doc), None

    online, _ = lax.scan(
        scan_step,
        online,
        (
            key_part.reshape(token_blocks, block_rows, heads_kv, HEAD_SIZE),
            value_part.reshape(token_blocks, block_rows, heads_kv, HEAD_SIZE),
            key_pos.reshape(token_blocks, block_rows),
            key_doc.reshape(token_blocks, block_rows),
        ),
    )
    return online


def general(queries, keys, values, doc_blocks, block_order, out_weight):
    rows_dev = queries.shape[0]
    heads_kv = keys.shape[1] // HEAD_SIZE
    group_size = queries.shape[1] // keys.shape[1]
    doc_ends = jnp.cumsum(doc_blocks)
    first_row = lax.axis_index("cp") * rows_dev
    query_pos, query_doc = locate(
        first_row + jnp.arange(rows_dev, dtype=jnp.int32), block_order, doc_ends
    )
    query_rows = queries.reshape(rows_dev, heads_kv, group_size, HEAD_SIZE)
    starting_state = (
        jnp.full((heads_kv, group_size, rows_dev), MASKED, jnp.float32),
        jnp.zeros((heads_kv, group_size, rows_dev), jnp.float32),
        jnp.zeros((heads_kv, group_size, rows_dev, HEAD_SIZE), jnp.float32),
    )
    whole_keys = lax.all_gather(keys, "cp", axis=0, tiled=True)
    whole_values = lax.all_gather(values, "cp", axis=0, tiled=True)
    _, weight_sum, weighted = sweep_keys(
        starting_state, whole_keys, whole_values, block_order, doc_ends,
        query_rows, query_pos, query_doc,
    )
    attended = (
        jnp.transpose(weighted / weight_sum[..., None], (2, 0, 1, 3))
        .reshape(rows_dev, -1)
        .astype(jnp.bfloat16)
    )
    return lax.psum_scatter(
        jnp.dot(attended, out_weight, preferred_element_type=jnp.float32).astype(jnp.bfloat16),
        "tp",
        scatter_dimension=0,
        tiled=True,
    )


def spread(x, width):
    return jnp.concatenate([x] * (width // x.shape[1]), 1)


def online(top_ref, sum_ref, at, queries, key_rows, value_rows, bias, fresh=False):
    scores = lax.dot_general(
        queries, key_rows, (((1,), (1,)), ((), ())), preferred_element_type=jnp.float32
    )
    if bias is not None:
        scores = scores + bias
    top = jnp.broadcast_to(jnp.max(scores, axis=1, keepdims=True), (scores.shape[0], HEAD_SIZE))
    if not fresh:
        before = top_ref[at, :]
        top = jnp.maximum(top, before)
    weights = jnp.exp2((scores - spread(top, scores.shape[1])) * SCALE).astype(jnp.bfloat16)
    sums = jnp.dot(weights, value_rows, preferred_element_type=jnp.float32)
    if not fresh:
        sums = sums + sum_ref[at, :] * spread(jnp.exp2((before - top) * SCALE), sums.shape[1])
    top_ref[at, :] = top
    sum_ref[at, :] = sums


def sweep(qr_ref, top_ref, sum_ref, kvs, bias, fresh=False):
    heads_kv = kvs[0].shape[1] // HEAD_SIZE
    height = qr_ref.shape[0] // heads_kv
    for g in range(heads_kv):
        cols = slice(g * HEAD_SIZE, (g + 1) * HEAD_SIZE)
        key_rows = jnp.concatenate([ref[:BLOCK_TOKENS, cols] for ref in kvs], 0)
        value_rows = jnp.concatenate([ref[BLOCK_TOKENS:, cols] for ref in kvs], 0)
        value_rows = jnp.concatenate([value_rows, jnp.ones_like(value_rows)], 1)
        at = pl.ds(g * height, height)
        online(top_ref, sum_ref, at, qr_ref[at, :], key_rows, value_rows, bias, fresh)


def start_all(copies):
    for copy in copies:
        copy.start()
    return copies


def wait_all(copies):
    for copy in copies:
        copy.wait()


def load_rows(src, first, out, sems):
    pieces = sems.shape[0]
    rows = out.shape[0] // pieces
    return start_all([
        pltpu.make_async_copy(
            src.at[pl.ds(first + i * rows, rows)], out.at[pl.ds(i * rows, rows)], sems.at[i])
        for i in range(pieces)
    ])


def begin(n_tp, order_hbm, docs_hbm, q_hbm, w_hbm, kv_ref, qr_ref, seen_ref, top_ref, sum_ref, w_ref,
          q_ref, order_ref, docs_ref, sems, w_sems):
    copies = start_all([
        pltpu.make_async_copy(src, dst, sems.at[i])
        for i, (src, dst) in enumerate(
            ((order_hbm, order_ref), (docs_hbm, docs_ref), (q_hbm, q_ref)))
    ])
    loads = load_rows(w_hbm, 0, w_ref, w_sems)
    wait_all(copies)
    n_blocks, n_docs = order_ref.shape[0], docs_ref.shape[0]
    rows, width = q_ref.shape
    part = rows // n_tp
    me, core = lax.axis_index("cp"), lax.axis_index("tp")
    ends = []
    for d in range(n_docs):
        ends.append(docs_ref[d] + (ends[-1] if ends else 0))

    def document(seq):
        return sum((seq >= end).astype(jnp.int32) for end in ends)

    own_seq = order_ref[me]
    own_doc = document(own_seq)
    for s in range(n_blocks):
        seq = order_ref[me ^ s]
        seen = (document(seq) == own_doc) & (seq < own_seq)
        seen_ref[s : s + 1, :] = jnp.full((1, HEAD_SIZE), seen.astype(jnp.int32), jnp.int32)

    targets = [core ^ f for f in (3, 1, 2, 0)]
    for h in range(width // HEAD_SIZE):
        for p, target in enumerate(targets):
            qr_ref[h * rows + p * part : h * rows + (p + 1) * part, :] = q_ref[
                pl.ds(pl.multiple_of(target * part, part), part),
                h * HEAD_SIZE : (h + 1) * HEAD_SIZE]
    key_at = lax.broadcasted_iota(jnp.int32, (part, BLOCK_TOKENS), 1)
    row_at = lax.broadcasted_iota(jnp.int32, (part, BLOCK_TOKENS), 0)
    bias = jnp.concatenate(
        [jnp.where(key_at <= row_at + target * part, 0.0, MASKED) for target in targets], 0)
    heads = width // kv_ref.shape[1]
    sweep(qr_ref, top_ref, sum_ref, [kv_ref], jnp.concatenate([bias] * heads, 0), fresh=True)
    wait_all(loads)


def seen_blocks(slots, seen_ref, qr_ref, top_ref, sum_ref, kv_refs, kv_ref):
    used = jnp.int32(0)
    for s, ref in zip(slots, kv_refs):
        wanted = jnp.max(seen_ref[s : s + 1, :])

        @pl.when(wanted == 1)
        def _(ref=ref, used=used):
            kv_ref[used] = ref[...]

        used = used + wanted
    for first in range(0, kv_ref.shape[0], 2):
        for count in (1, 2):
            if first + count > kv_ref.shape[0]:
                continue
            last = first + count == kv_ref.shape[0]

            @pl.when((used >= first + 2) if count == 2 else (used == first + 1))
            def _(first=first, count=count):
                sweep(qr_ref, top_ref, sum_ref, [kv_ref.at[first + i] for i in range(count)], None)


def more(slots, first, seen_ref, w_hbm, qr_ref, top_in, sum_in, *refs):
    kv_refs, (top_ref, sum_ref, w_ref, kv_ref, w_sems) = (
        refs[: len(slots)], refs[len(slots) :])
    loads = load_rows(w_hbm, first, w_ref, w_sems)
    seen_blocks(slots, seen_ref, qr_ref, top_ref, sum_ref, kv_refs, kv_ref)
    wait_all(loads)


def project(att_ref, w_refs, first, chunk, give_ref, keep_ref):
    half = att_ref.shape[0] // 2
    for j in range(give_ref.shape[1] // chunk):
        product, depth = None, 0
        for w_ref in w_refs:
            term = jnp.dot(
                att_ref[:, depth : depth + w_ref.shape[0]],
                w_ref[:, first + j * chunk : first + (j + 1) * chunk],
                preferred_element_type=jnp.float32)
            product = term if product is None else product + term
            depth += w_ref.shape[0]
        give_ref[:, j * chunk : (j + 1) * chunk] = product[:half].astype(jnp.bfloat16)
        keep_ref[:, j * chunk : (j + 1) * chunk] = product[half:]


def finish(slots, chunk, seen_ref, qr_ref, top_in, sum_in, *refs):
    kv_refs, w_refs, (top_ref, sum_ref, att_ref, give_ref, keep_ref, kv_ref) = (
        refs[: len(slots)], refs[len(slots) : -6], refs[-6:])
    seen_blocks(slots, seen_ref, qr_ref, top_ref, sum_ref, kv_refs, kv_ref)
    rows, width = att_ref.shape
    for h in range(width // HEAD_SIZE):
        at = slice(h * rows, (h + 1) * rows)
        att_ref[:, h * HEAD_SIZE : (h + 1) * HEAD_SIZE] = (
            sum_ref[at, :HEAD_SIZE] * pl.reciprocal(sum_ref[at, HEAD_SIZE:])
        ).astype(jnp.bfloat16)
    project(att_ref, w_refs, 0, chunk, give_ref, keep_ref)


def rest(chunk, att_ref, *refs):
    w_refs, (give_ref, keep_ref) = refs[:-2], refs[-2:]
    project(att_ref, w_refs, w_refs[0].shape[1] - give_ref.shape[1], chunk, give_ref, keep_ref)


def last(at, keep_ref, other_ref, crossed_ref, *refs):
    out_hbm, out_ref, sem = refs[-3:]
    part, width = out_ref.shape
    out_ref[...] = (
        keep_ref[part:] + other_ref[part:].astype(jnp.float32) + crossed_ref[...].astype(jnp.float32)
    ).astype(out_ref.dtype)
    wait_all(start_all([pltpu.make_async_copy(out_ref, out_hbm.at[:, pl.ds(at, width)], sem)]))


def in_hbm(x):
    return pltpu.with_memory_space_constraint(x, pltpu.HBM)


def in_vmem(x):
    return pltpu.with_memory_space_constraint(x, pltpu.VMEM)


HBM = pl.BlockSpec(memory_space=pltpu.HBM)
VMEM = pl.BlockSpec(memory_space=pltpu.VMEM)


def kernel(body, inputs, outs, scratch=(), flops=0, aliases={}, limit=16):
    return pl.pallas_call(
        body,
        out_shape=tuple(pltpu.VMEM(shape, dtype) for shape, dtype in outs),
        in_specs=[HBM if where == "hbm" else VMEM for where, _ in inputs],
        out_specs=(VMEM,) * len(outs),
        scratch_shapes=list(scratch),
        input_output_aliases=aliases,
        compiler_params=pltpu.CompilerParams(vmem_limit_bytes=limit * 1024 * 1024),
        cost_estimate=pl.CostEstimate(flops=flops, bytes_accessed=0, transcendentals=0),
    )(*[in_hbm(x) if where == "hbm" else in_vmem(x) for where, x in inputs])


def stack_kernel(k_hbm, v_hbm, out_ref, sems):
    rows = k_hbm.shape[0]
    copies = [
        pltpu.make_async_copy(k_hbm, out_ref.at[:rows], sems.at[0]),
        pltpu.make_async_copy(v_hbm, out_ref.at[rows:], sems.at[1]),
    ]
    for copy in copies:
        copy.start()
    for copy in copies:
        copy.wait()


SHARES = (3, 4, 1)
PLAN = ((4, 0, 4), (2, 0, 2), (1, 0, 1), (7, 0, 7), (3, 2, 1), (6, 4, 2), (5, 4, 1))


def blockwise(n, n_tp, queries, keys, values, doc_blocks, block_order, out_weight):
    rows, width = queries.shape
    heads = width // HEAD_SIZE
    out_width = out_weight.shape[1]
    bf16, f32 = jnp.bfloat16, jnp.float32

    def swap(block, s):
        return lax.ppermute(block, "cp", [(i, i ^ s) for i in range(n)])

    (kv,) = kernel(
        stack_kernel, [("hbm", keys), ("hbm", values)],
        [((2 * rows, keys.shape[1]), bf16)], [pltpu.SemaphoreType.DMA((2,))])
    got = {0: kv}
    for s, via, hop in PLAN:
        got[s] = swap(got[via], hop)

    states = [((heads * rows, HEAD_SIZE), f32), ((heads * rows, 2 * HEAD_SIZE), f32)]
    split = [width * share // 8 for share in SHARES]
    dma = pltpu.SemaphoreType.DMA
    qr, seen, top, sums, weight = kernel(
        functools.partial(begin, n_tp),
        [("hbm", block_order), ("hbm", doc_blocks), ("hbm", queries), ("hbm", out_weight), ("vmem", kv)],
        [((heads * rows, HEAD_SIZE), bf16), ((n, HEAD_SIZE), jnp.int32)] + states + [((split[0], out_width), bf16)],
        [pltpu.VMEM((rows, width), bf16), pltpu.SMEM(block_order.shape, jnp.int32),
         pltpu.SMEM(doc_blocks.shape, jnp.int32), dma((3,)), dma((split[0] // 128,))],
        flops=4 * 10**9, limit=8)

    def held(slots):
        return pltpu.VMEM((min(len(slots), n // 2 - 1),) + kv.shape, bf16)

    weights = [weight]
    for slots, depth in zip(((1, 2, 4), (3, 7, 6)), split[1:]):
        first = sum(w.shape[0] for w in weights)
        top, sums, weight = kernel(
            functools.partial(more, slots, first),
            [("vmem", seen), ("hbm", out_weight)]
            + [("vmem", x) for x in (qr, top, sums, *(got[s] for s in slots))],
            states + [((depth, out_width), bf16)], [held(slots), dma((depth // 128,))],
            flops=4 * 10**9, aliases={3: 0, 4: 1}, limit=8)
        weights.append(weight)
    slots = (5,)
    part, chunk, half = rows // n_tp, 512, out_width // 2
    shares = [((rows // 2, half), bf16), ((rows // 2, half), f32)]
    _, _, att, give0, keep0 = kernel(
        functools.partial(finish, slots, chunk),
        [("vmem", x) for x in (seen, qr, top, sums, *(got[s] for s in slots), *weights)],
        states + [((rows, width), bf16)] + shares, [held(slots)],
        flops=rows * width * out_width, aliases={2: 0, 3: 1}, limit=8)

    def across(x, hop):
        return lax.ppermute(x, "tp", [(i, i ^ hop) for i in range(n_tp)])

    got0 = across(give0, 1)
    give1, keep1 = kernel(
        functools.partial(rest, chunk), [("vmem", x) for x in (att, *weights)],
        shares, flops=rows * width * out_width, limit=8)
    got1 = across(give1, 1)
    crossed = []
    for keep, other in ((keep0, got0), (keep1, got1)):
        far = (keep[:part] + other[:part].astype(f32)).astype(bf16)
        crossed.append(across(far, 2))
    ends = ((keep0, got0, crossed[0]), (keep1, got1, crossed[1]))
    out = ()
    for i, terms in enumerate(ends):
        out = pl.pallas_call(
            functools.partial(last, i * half),
            out_shape=(pltpu.HBM((part, out_width), bf16),),
            in_specs=[VMEM] * 3 + [HBM] * len(out),
            out_specs=(HBM,),
            scratch_shapes=[pltpu.VMEM((part, half), bf16), dma(())],
            input_output_aliases={3: 0} if out else {},
            compiler_params=pltpu.CompilerParams(vmem_limit_bytes=8 * 1024 * 1024),
        )(*map(in_vmem, terms), *out)
    return out[0]


def solution(mesh):
    n, n_tp = mesh.shape["cp"], mesh.shape["tp"]

    def local(queries, keys, values, doc_blocks, block_order, out_weight):
        args = (queries, keys, values, doc_blocks, block_order, out_weight)
        if n == 8 and n_tp == 4:
            return blockwise(n, n_tp, *args)
        return general(*args)

    placed = (P("cp", "tp"), P("cp", "tp"), P("cp", "tp"), P(), P(), P("tp", None))
    return jax.shard_map(
        local, mesh=mesh, in_specs=placed, out_specs=P(("cp", "tp"), None), check_vma=False
    )
```

```python
import functools

import jax
import jax.numpy as jnp
from jax import lax
from jax.experimental import pallas as pl
from jax.experimental.pallas import tpu as pltpu
from jax.sharding import PartitionSpec as P


HEAD_SIZE = 128
BLOCK_TOKENS = 128
MASKED = -1e30
SCALE = HEAD_SIZE**-0.5 * 1.4426950408889634


def lookup(entries, indices):
    matches = indices[:, None] == jnp.arange(entries.shape[0], dtype=jnp.int32)[None, :]
    return jnp.sum(jnp.where(matches, entries[None, :], 0), axis=1)


def locate(row_ids, block_order, doc_ends):
    seq_block = lookup(block_order, row_ids // BLOCK_TOKENS)
    position = seq_block * BLOCK_TOKENS + row_ids % BLOCK_TOKENS
    doc_ids = jnp.sum((seq_block[:, None] >= doc_ends[None, :]).astype(jnp.int32), axis=1)
    return (position, doc_ids)


def attend(online, key_rows, value_rows, key_pos, key_doc, query_rows, query_pos, query_doc):
    allowed = (query_doc[:, None] == key_doc[None, :]) & (key_pos[None, :] <= query_pos[:, None])
    running_max, weight_sum, weighted = online
    scores = jnp.einsum(
        "qhgd,khd->hgqk", query_rows, key_rows, preferred_element_type=jnp.float32
    ) * HEAD_SIZE ** (-0.5)
    scores = jnp.where(allowed, scores, MASKED)
    new_max = jnp.maximum(running_max, jnp.max(scores, axis=-1))
    weights = jnp.where(allowed, jnp.exp(scores - new_max[..., None]), 0.0)
    factor = jnp.exp(running_max - new_max)
    weight_sum = weight_sum * factor + jnp.sum(weights, axis=-1)
    weighted = weighted * factor[..., None] + jnp.einsum(
        "hgqk,khd->hgqd",
        weights.astype(jnp.bfloat16),
        value_rows,
        preferred_element_type=jnp.float32,
    )
    return (new_max, weight_sum, weighted)


def sweep_keys(
    online, key_part, value_part, block_order, doc_ends, query_rows, query_pos, query_doc
):
    length = key_part.shape[0]
    heads_kv = key_part.shape[1] // HEAD_SIZE
    block_rows = 4 * BLOCK_TOKENS
    token_blocks = length // block_rows
    key_pos, key_doc = locate(jnp.arange(length, dtype=jnp.int32), block_order, doc_ends)

    def scan_step(status, pieces_now):
        return attend(status, *pieces_now, query_rows, query_pos, query_doc), None

    online, _ = lax.scan(
        scan_step,
        online,
        (
            key_part.reshape(token_blocks, block_rows, heads_kv, HEAD_SIZE),
            value_part.reshape(token_blocks, block_rows, heads_kv, HEAD_SIZE),
            key_pos.reshape(token_blocks, block_rows),
            key_doc.reshape(token_blocks, block_rows),
        ),
    )
    return online


def general(queries, keys, values, doc_blocks, block_order, out_weight):
    rows_dev = queries.shape[0]
    heads_kv = keys.shape[1] // HEAD_SIZE
    group_size = queries.shape[1] // keys.shape[1]
    doc_ends = jnp.cumsum(doc_blocks)
    first_row = lax.axis_index("cp") * rows_dev
    query_pos, query_doc = locate(
        first_row + jnp.arange(rows_dev, dtype=jnp.int32), block_order, doc_ends
    )
    query_rows = queries.reshape(rows_dev, heads_kv, group_size, HEAD_SIZE)
    starting_state = (
        jnp.full((heads_kv, group_size, rows_dev), MASKED, jnp.float32),
        jnp.zeros((heads_kv, group_size, rows_dev), jnp.float32),
        jnp.zeros((heads_kv, group_size, rows_dev, HEAD_SIZE), jnp.float32),
    )
    whole_keys = lax.all_gather(keys, "cp", axis=0, tiled=True)
    whole_values = lax.all_gather(values, "cp", axis=0, tiled=True)
    _, weight_sum, weighted = sweep_keys(
        starting_state, whole_keys, whole_values, block_order, doc_ends,
        query_rows, query_pos, query_doc,
    )
    attended = (
        jnp.transpose(weighted / weight_sum[..., None], (2, 0, 1, 3))
        .reshape(rows_dev, -1)
        .astype(jnp.bfloat16)
    )
    return lax.psum_scatter(
        jnp.dot(attended, out_weight, preferred_element_type=jnp.float32).astype(jnp.bfloat16),
        "tp",
        scatter_dimension=0,
        tiled=True,
    )


def spread(x, width):
    return jnp.concatenate([x] * (width // x.shape[1]), 1)


def online(top_ref, sum_ref, at, queries, key_rows, value_rows, bias, fresh=False):
    scores = lax.dot_general(
        queries, key_rows, (((1,), (1,)), ((), ())), preferred_element_type=jnp.float32
    )
    if bias is not None:
        scores = scores + bias
    top = jnp.broadcast_to(jnp.max(scores, axis=1, keepdims=True), (scores.shape[0], HEAD_SIZE))
    if not fresh:
        before = top_ref[at, :]
        top = jnp.maximum(top, before)
    weights = jnp.exp2((scores - spread(top, scores.shape[1])) * SCALE).astype(jnp.bfloat16)
    sums = jnp.dot(weights, value_rows, preferred_element_type=jnp.float32)
    if not fresh:
        sums = sums + sum_ref[at, :] * spread(jnp.exp2((before - top) * SCALE), sums.shape[1])
    top_ref[at, :] = top
    sum_ref[at, :] = sums


def sweep(qr_ref, top_ref, sum_ref, kvs, bias, fresh=False):
    heads_kv = kvs[0].shape[1] // HEAD_SIZE
    height = qr_ref.shape[0] // heads_kv
    for g in range(heads_kv):
        cols = slice(g * HEAD_SIZE, (g + 1) * HEAD_SIZE)
        key_rows = jnp.concatenate([ref[:BLOCK_TOKENS, cols] for ref in kvs], 0)
        value_rows = jnp.concatenate([ref[BLOCK_TOKENS:, cols] for ref in kvs], 0)
        value_rows = jnp.concatenate([value_rows, jnp.ones_like(value_rows)], 1)
        at = pl.ds(g * height, height)
        online(top_ref, sum_ref, at, qr_ref[at, :], key_rows, value_rows, bias, fresh)


def start_all(copies):
    for copy in copies:
        copy.start()
    return copies


def wait_all(copies):
    for copy in copies:
        copy.wait()


def load_rows(src, first, out, sems):
    pieces = sems.shape[0]
    rows = out.shape[0] // pieces
    return start_all([
        pltpu.make_async_copy(
            src.at[pl.ds(first + i * rows, rows)], out.at[pl.ds(i * rows, rows)], sems.at[i])
        for i in range(pieces)
    ])


def begin(n_tp, order_hbm, docs_hbm, q_hbm, w_hbm, kv_ref, qr_ref, seen_ref, top_ref, sum_ref, w_ref,
          q_ref, order_ref, docs_ref, sems, w_sems):
    copies = start_all([
        pltpu.make_async_copy(src, dst, sems.at[i])
        for i, (src, dst) in enumerate(
            ((order_hbm, order_ref), (docs_hbm, docs_ref), (q_hbm, q_ref)))
    ])
    loads = load_rows(w_hbm, 0, w_ref, w_sems)
    wait_all(copies)
    n_blocks, n_docs = order_ref.shape[0], docs_ref.shape[0]
    rows, width = q_ref.shape
    part = rows // n_tp
    me, core = lax.axis_index("cp"), lax.axis_index("tp")
    ends = []
    for d in range(n_docs):
        ends.append(docs_ref[d] + (ends[-1] if ends else 0))

    def document(seq):
        return sum((seq >= end).astype(jnp.int32) for end in ends)

    own_seq = order_ref[me]
    own_doc = document(own_seq)
    for s in range(n_blocks):
        seq = order_ref[me ^ s]
        seen = (document(seq) == own_doc) & (seq < own_seq)
        seen_ref[s : s + 1, :] = jnp.full((1, HEAD_SIZE), seen.astype(jnp.int32), jnp.int32)

    targets = [core ^ f for f in (3, 1, 2, 0)]
    for h in range(width // HEAD_SIZE):
        for p, target in enumerate(targets):
            qr_ref[h * rows + p * part : h * rows + (p + 1) * part, :] = q_ref[
                pl.ds(pl.multiple_of(target * part, part), part),
                h * HEAD_SIZE : (h + 1) * HEAD_SIZE]
    key_at = lax.broadcasted_iota(jnp.int32, (part, BLOCK_TOKENS), 1)
    row_at = lax.broadcasted_iota(jnp.int32, (part, BLOCK_TOKENS), 0)
    bias = jnp.concatenate(
        [jnp.where(key_at <= row_at + target * part, 0.0, MASKED) for target in targets], 0)
    heads = width // kv_ref.shape[1]
    sweep(qr_ref, top_ref, sum_ref, [kv_ref], jnp.concatenate([bias] * heads, 0), fresh=True)
    wait_all(loads)


def seen_blocks(slots, seen_ref, qr_ref, top_ref, sum_ref, kv_refs, kv_ref):
    used = jnp.int32(0)
    for s, ref in zip(slots, kv_refs):
        wanted = jnp.max(seen_ref[s : s + 1, :])

        @pl.when(wanted == 1)
        def _(ref=ref, used=used):
            kv_ref[used] = ref[...]

        used = used + wanted
    for first in range(0, kv_ref.shape[0], 2):
        for count in (1, 2):
            if first + count > kv_ref.shape[0]:
                continue
            last = first + count == kv_ref.shape[0]

            @pl.when((used >= first + 2) if count == 2 else (used == first + 1))
            def _(first=first, count=count):
                sweep(qr_ref, top_ref, sum_ref, [kv_ref.at[first + i] for i in range(count)], None)


def more(slots, first, seen_ref, w_hbm, qr_ref, top_in, sum_in, *refs):
    kv_refs, (top_ref, sum_ref, w_ref, kv_ref, w_sems) = (
        refs[: len(slots)], refs[len(slots) :])
    loads = load_rows(w_hbm, first, w_ref, w_sems)
    seen_blocks(slots, seen_ref, qr_ref, top_ref, sum_ref, kv_refs, kv_ref)
    wait_all(loads)


def project(att_ref, w_refs, first, chunk, give_ref, keep_ref):
    half = att_ref.shape[0] // 2
    for j in range(give_ref.shape[1] // chunk):
        product, depth = None, 0
        for w_ref in w_refs:
            term = jnp.dot(
                att_ref[:, depth : depth + w_ref.shape[0]],
                w_ref[:, first + j * chunk : first + (j + 1) * chunk],
                preferred_element_type=jnp.float32)
            product = term if product is None else product + term
            depth += w_ref.shape[0]
        give_ref[:, j * chunk : (j + 1) * chunk] = product[:half].astype(jnp.bfloat16)
        keep_ref[:, j * chunk : (j + 1) * chunk] = product[half:]


def finish(slots, chunk, seen_ref, qr_ref, top_in, sum_in, *refs):
    kv_refs, w_refs, (top_ref, sum_ref, att_ref, give_ref, keep_ref, kv_ref) = (
        refs[: len(slots)], refs[len(slots) : -6], refs[-6:])
    seen_blocks(slots, seen_ref, qr_ref, top_ref, sum_ref, kv_refs, kv_ref)
    rows, width = att_ref.shape
    for h in range(width // HEAD_SIZE):
        at = slice(h * rows, (h + 1) * rows)
        att_ref[:, h * HEAD_SIZE : (h + 1) * HEAD_SIZE] = (
            sum_ref[at, :HEAD_SIZE] * pl.reciprocal(sum_ref[at, HEAD_SIZE:])
        ).astype(jnp.bfloat16)
    project(att_ref, w_refs, 0, chunk, give_ref, keep_ref)


def rest(chunk, att_ref, *refs):
    w_refs, (give_ref, keep_ref) = refs[:-2], refs[-2:]
    project(att_ref, w_refs, w_refs[0].shape[1] - give_ref.shape[1], chunk, give_ref, keep_ref)


def last(at, keep_ref, other_ref, crossed_ref, *refs):
    out_hbm, out_ref, sem = refs[-3:]
    part, width = out_ref.shape
    out_ref[...] = (
        keep_ref[part:] + other_ref[part:].astype(jnp.float32) + crossed_ref[...].astype(jnp.float32)
    ).astype(out_ref.dtype)
    wait_all(start_all([pltpu.make_async_copy(out_ref, out_hbm.at[:, pl.ds(at, width)], sem)]))


def in_hbm(x):
    return pltpu.with_memory_space_constraint(x, pltpu.HBM)


def in_vmem(x):
    return pltpu.with_memory_space_constraint(x, pltpu.VMEM)


HBM = pl.BlockSpec(memory_space=pltpu.HBM)
VMEM = pl.BlockSpec(memory_space=pltpu.VMEM)


def kernel(body, inputs, outs, scratch=(), flops=0, aliases={}, limit=16):
    return pl.pallas_call(
        body,
        out_shape=tuple(pltpu.VMEM(shape, dtype) for shape, dtype in outs),
        in_specs=[HBM if where == "hbm" else VMEM for where, _ in inputs],
        out_specs=(VMEM,) * len(outs),
        scratch_shapes=list(scratch),
        input_output_aliases=aliases,
        compiler_params=pltpu.CompilerParams(vmem_limit_bytes=limit * 1024 * 1024),
        cost_estimate=pl.CostEstimate(flops=flops, bytes_accessed=0, transcendentals=0),
    )(*[in_hbm(x) if where == "hbm" else in_vmem(x) for where, x in inputs])


def stack_kernel(k_hbm, v_hbm, out_ref, sems):
    rows = k_hbm.shape[0]
    copies = [
        pltpu.make_async_copy(k_hbm, out_ref.at[:rows], sems.at[0]),
        pltpu.make_async_copy(v_hbm, out_ref.at[rows:], sems.at[1]),
    ]
    for copy in copies:
        copy.start()
    for copy in copies:
        copy.wait()


SHARES = (3, 4, 1)
PLAN = ((3, 0, 3), (4, 0, 4), (2, 0, 2), (1, 0, 1), (7, 0, 7), (5, 4, 1), (6, 4, 2))


def blockwise(n, n_tp, queries, keys, values, doc_blocks, block_order, out_weight):
    rows, width = queries.shape
    heads = width // HEAD_SIZE
    out_width = out_weight.shape[1]
    bf16, f32 = jnp.bfloat16, jnp.float32

    def swap(block, s):
        return lax.ppermute(block, "cp", [(i, i ^ s) for i in range(n)])

    (kv,) = kernel(
        stack_kernel, [("hbm", keys), ("hbm", values)],
        [((2 * rows, keys.shape[1]), bf16)], [pltpu.SemaphoreType.DMA((2,))])
    got = {0: kv}
    for s, via, hop in PLAN:
        got[s] = swap(got[via], hop)

    states = [((heads * rows, HEAD_SIZE), f32), ((heads * rows, 2 * HEAD_SIZE), f32)]
    split = [width * share // 8 for share in SHARES]
    dma = pltpu.SemaphoreType.DMA
    qr, seen, top, sums, weight = kernel(
        functools.partial(begin, n_tp),
        [("hbm", block_order), ("hbm", doc_blocks), ("hbm", queries), ("hbm", out_weight), ("vmem", kv)],
        [((heads * rows, HEAD_SIZE), bf16), ((n, HEAD_SIZE), jnp.int32)] + states + [((split[0], out_width), bf16)],
        [pltpu.VMEM((rows, width), bf16), pltpu.SMEM(block_order.shape, jnp.int32),
         pltpu.SMEM(doc_blocks.shape, jnp.int32), dma((3,)), dma((split[0] // 128,))],
        flops=4 * 10**9, limit=8)

    def held(slots):
        return pltpu.VMEM((min(len(slots), n // 2 - 1),) + kv.shape, bf16)

    weights = [weight]
    for slots, depth in zip(((1, 2, 4), (3, 7, 5)), split[1:]):
        first = sum(w.shape[0] for w in weights)
        top, sums, weight = kernel(
            functools.partial(more, slots, first),
            [("vmem", seen), ("hbm", out_weight)]
            + [("vmem", x) for x in (qr, top, sums, *(got[s] for s in slots))],
            states + [((depth, out_width), bf16)], [held(slots), dma((depth // 128,))],
            flops=4 * 10**9, aliases={3: 0, 4: 1}, limit=8)
        weights.append(weight)
    slots = (6,)
    part, chunk, half = rows // n_tp, 512, out_width // 2
    shares = [((rows // 2, half), bf16), ((rows // 2, half), f32)]
    _, _, att, give0, keep0 = kernel(
        functools.partial(finish, slots, chunk),
        [("vmem", x) for x in (seen, qr, top, sums, *(got[s] for s in slots), *weights)],
        states + [((rows, width), bf16)] + shares, [held(slots)],
        flops=rows * width * out_width, aliases={2: 0, 3: 1}, limit=8)

    def across(x, hop):
        return lax.ppermute(x, "tp", [(i, i ^ hop) for i in range(n_tp)])

    got0 = across(give0, 1)
    give1, keep1 = kernel(
        functools.partial(rest, chunk), [("vmem", x) for x in (att, *weights)],
        shares, flops=rows * width * out_width, limit=8)
    got1 = across(give1, 1)
    crossed = []
    for keep, other in ((keep0, got0), (keep1, got1)):
        far = (keep[:part] + other[:part].astype(f32)).astype(bf16)
        crossed.append(across(far, 2))
    ends = ((keep0, got0, crossed[0]), (keep1, got1, crossed[1]))
    out = ()
    for i, terms in enumerate(ends):
        out = pl.pallas_call(
            functools.partial(last, i * half),
            out_shape=(pltpu.HBM((part, out_width), bf16),),
            in_specs=[VMEM] * 3 + [HBM] * len(out),
            out_specs=(HBM,),
            scratch_shapes=[pltpu.VMEM((part, half), bf16), dma(())],
            input_output_aliases={3: 0} if out else {},
            compiler_params=pltpu.CompilerParams(vmem_limit_bytes=8 * 1024 * 1024),
        )(*map(in_vmem, terms), *out)
    return out[0]


def solution(mesh):
    n, n_tp = mesh.shape["cp"], mesh.shape["tp"]

    def local(queries, keys, values, doc_blocks, block_order, out_weight):
        args = (queries, keys, values, doc_blocks, block_order, out_weight)
        if n == 8 and n_tp == 4:
            return blockwise(n, n_tp, *args)
        return general(*args)

    placed = (P("cp", "tp"), P("cp", "tp"), P("cp", "tp"), P(), P(), P("tp", None))
    return jax.shard_map(
        local, mesh=mesh, in_specs=placed, out_specs=P(("cp", "tp"), None), check_vma=False
    )
```
